256 devices in a mesh: seq: 16 (over y_hi, z), head: 16 (over y_lo, x, core).
Axes of the slice: x: 4, y: 4 (y_hi: 2, y_lo: 2; y = y_hi * 2 + y_lo), z: 8, core: 2. Of those that a mesh axis runs over, the one named last changes fastest.
Arguments:
- queries: bfloat16 [16384, 4096], P(('seq', 'head')), may hold values from -9 to 9, as said below
- keys: bfloat16 [16384, 512], P(('seq', 'head')), may hold values from -9 to 9, as said below
- values: bfloat16 [16384, 512], P(('seq', 'head')), may hold values from -6 to 6
Outputs:
- attended: bfloat16 [16384, 4096], P(('seq', 'head'))
The draws below stay inside these ranges and needn't reach their ends.
Inputs may be any that keep to these rules, and one draw needn't show every extreme that they name: `queries`: query entries are of order one except on a few rows. `keys`: key entries are of order one except on a few rows.
All inputs are finite; a program needn't handle non-finite values.
Results may differ from the reference program's by a relative error of at most 0.005.
Values may be sent and summed in bfloat16 or wider, within the bound.
No kernel may reach another device: no remote copies, remote signals or barrier semaphores. Data moves between devices by JAX's collectives and lax.ppermute only.
A program may use at most 64 MiB of HBM per device.

```python
import math
import jax
import jax.numpy as jnp
from jax import lax

H = 32
KV = 4
DH = 128
TOKENS = 16384


def paired(key):
    base = jax.random.fold_in(key, 7)
    key_q, key_k = jax.random.split(base, 2)
    query_mat = jnp.clip(jax.random.normal(key_q, (TOKENS, H * DH), jnp.float32), -6.0, 6.0)
    key_mat = jnp.clip(jax.random.normal(key_k, (TOKENS, KV * DH), jnp.float32), -6.0, 6.0)
    return (query_mat, key_mat)


def draw_queries(key, part):
    return paired(key)[0].astype(jnp.bfloat16)


def draw_keys(key, part):
    return paired(key)[1].astype(jnp.bfloat16)


def shard_levels(key, dims, pieces, smallest, high):
    factor_of, own = 1.0, jax.random.fold_in(key, 6)
    for position, shards_of in pieces:
        draws = jnp.exp(jax.random.uniform(jax.random.fold_in(own, position), (shards_of,), jnp.float32, smallest / len(pieces), high / len(pieces)))
        factor_of = factor_of * jnp.repeat(draws, dims[position] // shards_of).reshape([-1 if axis == position else 1 for axis in range(len(dims))])
    return factor_of


def scatter_about(rng, dims, spread, bound, shards=(), kind=jnp.bfloat16):
    array = spread * jax.random.normal(rng, dims, jnp.float32)
    if shards:
        array = array * shard_levels(rng, dims, shards, -0.22, 0.18)
    return jnp.clip(array, -bound, bound).astype(kind)


def setup_inputs(seed: int = 0) -> dict:
    seeds = jax.random.split(jax.random.key(seed), 4)
    queries = draw_queries(jax.random.fold_in(seeds[3], 71), 0)
    keys = draw_keys(jax.random.fold_in(seeds[3], 71), 0)
    values = scatter_about(seeds[2], (TOKENS, KV * DH), 1.0, 6.0, ((0, 256),))
    return dict(queries=queries, keys=keys, values=values)


def reference(queries, keys, values):
    length = queries.shape[0]
    block = min(1024, length)
    blocks = length // block
    group = H // KV
    scale = 1.0 / math.sqrt(DH)
    q_heads = queries.reshape(length, H, DH)
    k_heads = keys.reshape(length, KV, DH)
    v_heads = values.reshape(length, KV, DH)
    key_pos = jnp.arange(length, dtype=jnp.int32)

    def one_head(head):
        q_mat = lax.dynamic_index_in_dim(q_heads, head, 1, keepdims=False)
        k_mat = lax.dynamic_index_in_dim(k_heads, head // group, 1, keepdims=False)
        v_mat = lax.dynamic_index_in_dim(v_heads, head // group, 1, keepdims=False)

        def one_block(index):
            first = (index * block).astype(jnp.int32)
            rows = lax.dynamic_slice_in_dim(q_mat, first, block, 0)
            scores = jnp.dot(rows, k_mat.T, preferred_element_type=jnp.float32) * scale
            query_pos = first + jnp.arange(block, dtype=jnp.int32)
            scores = jnp.where(key_pos[None, :] <= query_pos[:, None], scores, -jnp.inf)
            rowmax = lax.optimization_barrier(jnp.max(scores, axis=1, keepdims=True))
            expo = jnp.exp(scores - rowmax)
            total = lax.optimization_barrier(jnp.sum(expo, axis=1, keepdims=True))
            numer = jnp.dot(expo.astype(jnp.bfloat16), v_mat, preferred_element_type=jnp.float32)
            return (numer / total).astype(jnp.bfloat16)
        return lax.map(one_block, jnp.arange(blocks, dtype=jnp.int32)).reshape(length, DH)
    result = lax.map(one_head, jnp.arange(H, dtype=jnp.int32))
    return result.transpose(1, 0, 2).reshape(length, H * DH)
```

```python
import functools
import math

import jax
import jax.numpy as jnp
from jax import lax
from jax.experimental import pallas as pl
from jax.experimental.pallas import tpu as pltpu
from jax.sharding import Mesh, PartitionSpec as P

H = 32
KV = 4
DH = 128
STRIP = 64
C2 = math.log2(math.e) / math.sqrt(DH)
NEG = -1e30
AXES = ("yh", "z", "yl", "x", "c")
VMEM = pl.BlockSpec(memory_space=pltpu.VMEM)
SMEM = pl.BlockSpec(memory_space=pltpu.SMEM)


def prep_kernel(kv_ref, out_ref):
    for half in range(2):
        base = half * 1024
        for s in range(8):
            src = half * 8 + s
            out_ref[base + s * 64 : base + (s + 1) * 64, :] = kv_ref[src, :64, :]
        for b in range(4):
            src = half * 8 + 2 * b
            block = jnp.concatenate([kv_ref[src, 64:, :], kv_ref[src + 1, 64:, :]], axis=0)
            at = base + 512 + b * 128
            out_ref[at : at + 128, :] = block.astype(jnp.float32).T.astype(jnp.bfloat16)


def prep(kv):
    return pl.pallas_call(
        prep_kernel,
        out_shape=jax.ShapeDtypeStruct((2048, DH), jnp.bfloat16),
        in_specs=[VMEM],
        out_specs=VMEM,
        name="prep",
        compiler_params=pltpu.CompilerParams(vmem_limit_bytes=8 * 1024 * 1024),
        cost_estimate=pl.CostEstimate(flops=1000000, bytes_accessed=1000000, transcendentals=0),
    )(kv)


def pair_unit(q_refs, acc_refs, st_refs, t, k_blk, vt_blk, mask_of):
    todo = [(w, hq) for w in range(2) for hq in range(2)]
    scores = []
    for w, hq in todo:
        rows = jnp.concatenate(
            [q_refs[w][t, :, (hq * 4 + i) * DH : (hq * 4 + i + 1) * DH] for i in range(4)], axis=0
        )
        s = lax.dot_general(k_blk, rows, (((1,), (1,)), ((), ())), preferred_element_type=jnp.float32)
        if mask_of is not None:
            s = jnp.where(mask_of(w, t), s, NEG)
        scores.append(s)
    for (w, hq), s in zip(todo, scores):
        m_old = st_refs[w][t, hq, 0:1, :]
        l_old = st_refs[w][t, hq, 1:2, :]
        m_new = jnp.maximum(m_old, jnp.max(s, axis=0, keepdims=True))
        mc = m_new * C2
        p = jnp.exp2(s * C2 - mc)
        alpha = jnp.exp2(m_old * C2 - mc)
        st_refs[w][t, hq, 0:1, :] = m_new
        st_refs[w][t, hq, 1:2, :] = alpha * l_old + jnp.sum(p, axis=0, keepdims=True)
        pv = lax.dot_general(
            vt_blk, p.astype(jnp.bfloat16), (((1,), (0,)), ((), ())), preferred_element_type=jnp.float32
        )
        acc_refs[w][t, hq] = alpha * acc_refs[w][t, hq] + pv


def blocks_of(ch_ref, half):
    base = half * 1024
    k_blk = ch_ref[base : base + 512, :]
    vt_blk = jnp.concatenate(
        [ch_ref[base + 512 + b * 128 : base + 512 + (b + 1) * 128, :] for b in range(4)], axis=1
    )
    return k_blk, vt_blk


def loop_tiles(lo, q_refs, acc_refs, st_refs, ch_ref, half, mask_of=None, hi=4):
    k_blk, vt_blk = blocks_of(ch_ref, half)

    def body(t, carry):
        pair_unit(q_refs, acc_refs, st_refs, t, k_blk, vt_blk, mask_of)
        return carry

    lax.fori_loop(lo, hi, body, 0)


def own_kernel(sc_ref, q0, q1, ch_ref, acc0, acc1, st0, st1):
    x, c = sc_ref[1], sc_ref[2]
    q_refs, acc_refs, st_refs = (q0, q1), (acc0, acc1), (st0, st1)
    row = lax.broadcasted_iota(jnp.int32, (1, 256), 1) % STRIP
    key = lax.broadcasted_iota(jnp.int32, (512, 1), 0)
    key_pos = (key // 256) * 512 + ((key % 256) // STRIP) * 128 + c * STRIP + key % STRIP

    def mask_of(w, t):
        core = c if w == 0 else 1 - c
        return key_pos <= (t % 2) * 512 + x * 128 + core * STRIP + row

    for w in range(2):
        acc_refs[w][...] = jnp.zeros_like(acc_refs[w])
        st_refs[w][:, :, 0:1, :] = jnp.full((4, 2, 1, 256), NEG, jnp.float32)
        st_refs[w][:, :, 1:2, :] = jnp.zeros((4, 2, 1, 256), jnp.float32)
    loop_tiles(0, q_refs, acc_refs, st_refs, ch_ref, 0, mask_of, 2)
    loop_tiles(2, q_refs, acc_refs, st_refs, ch_ref, 0)
    loop_tiles(2, q_refs, acc_refs, st_refs, ch_ref, 1, mask_of)


def step_kernel(parts, sc_ref, q0, q1, *refs):
    n = len(parts)
    chunks = refs[:n]
    acc_refs, st_refs = refs[n + 4 : n + 6], refs[n + 6 : n + 8]
    q_refs = (q0, q1)
    for ch_ref, (halves, at) in zip(chunks, parts):
        before = sc_ref[at]
        for slot, half in enumerate(halves):
            if half == 0:
                loop_tiles(2 - 2 * before, q_refs, acc_refs, st_refs, ch_ref, slot)
            else:
                loop_tiles(4 - 2 * before, q_refs, acc_refs, st_refs, ch_ref, slot)


ST = (
    jax.ShapeDtypeStruct((4, 2, DH, 256), jnp.float32),
    jax.ShapeDtypeStruct((4, 2, DH, 256), jnp.float32),
    jax.ShapeDtypeStruct((4, 2, 8, 256), jnp.float32),
    jax.ShapeDtypeStruct((4, 2, 8, 256), jnp.float32),
)


def cost(units):
    work = units * 8 * 512 * 256
    return pl.CostEstimate(flops=4 * work * DH, bytes_accessed=6000000, transcendentals=work)


def own_step(sc, q0, q1, chunk):
    return pl.pallas_call(
        own_kernel,
        out_shape=ST,
        in_specs=[SMEM, VMEM, VMEM, VMEM],
        out_specs=(VMEM,) * 4,
        name="own",
        compiler_params=pltpu.CompilerParams(vmem_limit_bytes=24 * 1024 * 1024),
        cost_estimate=cost(6),
    )(sc, q0, q1, chunk)


def ring_step(sc, q0, q1, state, chunks, parts):
    n = len(chunks)
    return pl.pallas_call(
        functools.partial(step_kernel, parts),
        out_shape=ST,
        in_specs=[SMEM, VMEM, VMEM] + [VMEM] * (n + 4),
        out_specs=(VMEM,) * 4,
        input_output_aliases={3 + n + i: i for i in range(4)},
        name="ring",
        compiler_params=pltpu.CompilerParams(vmem_limit_bytes=24 * 1024 * 1024),
        cost_estimate=cost(8),
    )(sc, q0, q1, *chunks, *state)


def merge_kernel(a_ref, s_ref, ra_ref, rs_ref, out_ref):
    for t in range(4):
        for hq in range(2):
            m0, l0 = s_ref[t, hq, 0:1, :], s_ref[t, hq, 1:2, :]
            m1, l1 = rs_ref[t, hq, 0:1, :], rs_ref[t, hq, 1:2, :]
            m = jnp.maximum(m0, m1)
            f0, f1 = jnp.exp2((m0 - m) * C2), jnp.exp2((m1 - m) * C2)
            total = f0 * l0 + f1 * l1
            out = (f0 * a_ref[t, hq] + f1 * ra_ref[t, hq]) / total
            rows = out.T.astype(jnp.bfloat16)
            for i in range(4):
                at = (hq * 4 + i) * DH
                out_ref[t, :, at : at + DH] = rows[i * STRIP : (i + 1) * STRIP, :]


def merge(acc, st, racc, rst):
    return pl.pallas_call(
        merge_kernel,
        out_shape=jax.ShapeDtypeStruct((4, STRIP, 8 * DH), jnp.bfloat16),
        in_specs=[VMEM] * 4,
        out_specs=VMEM,
        name="merge",
        compiler_params=pltpu.CompilerParams(vmem_limit_bytes=12 * 1024 * 1024),
        cost_estimate=pl.CostEstimate(flops=2000000, bytes_accessed=3000000, transcendentals=0),
    )(acc, st, racc, rst)


def per_device(queries, keys, values):
    z, x, c = lax.axis_index("z"), lax.axis_index("x"), lax.axis_index("c")
    k4 = keys.reshape(STRIP, KV, DH).transpose(1, 0, 2)
    v4 = values.reshape(STRIP, KV, DH).transpose(1, 0, 2)
    kv = jnp.concatenate([k4, v4], axis=1)
    kv = jnp.broadcast_to(kv[:, None], (KV, 4, 2 * STRIP, DH)).reshape(16, 2 * STRIP, DH)
    kv = lax.all_to_all(kv, ("yh", "yl", "x"), split_axis=0, concat_axis=0, tiled=True)
    chunk = prep(kv)

    q = queries.reshape(STRIP, KV, 8 * DH)
    q0 = lax.all_to_all(q, ("yh", "yl"), split_axis=1, concat_axis=0, tiled=True)
    q0 = q0.reshape(4, STRIP, 8 * DH)
    swap = [(0, 1), (1, 0)]
    q1 = lax.ppermute(q0, "c", swap)

    nz = lax.axis_size("z")
    up = [(i, (i + 1) % nz) for i in range(nz)]
    down = [(i, (i - 1) % nz) for i in range(nz)]
    fwd, bwd = [chunk], [chunk]
    for k in range(1, 4):
        fwd.append(lax.ppermute(fwd[-1], "z", up))
        bwd.append(lax.ppermute(bwd[-1], "z", down))
    far_l = lax.ppermute(fwd[3][:1024], "z", up)
    far_h = lax.ppermute(bwd[3][1024:], "z", down)

    flags = [(z - k >= 0).astype(jnp.int32) for k in range(5)]
    wraps = [(z + k >= nz).astype(jnp.int32) for k in range(5)]
    sc = jnp.stack([z, x, c, *flags[1:], *wraps[1:]]).astype(jnp.int32)

    state = own_step(sc, q0, q1, chunk)
    for k in range(1, 4):
        parts = (((0, 1), 2 + k), ((0, 1), 6 + k))
        state = ring_step(sc, q0, q1, state, (fwd[k], bwd[k]), parts)
    state = ring_step(sc, q0, q1, state, (far_l, far_h), (((0,), 6), ((1,), 6)))
    acc0, acc1, st0, st1 = state
    racc = lax.ppermute(acc1, "c", swap)
    rst = lax.ppermute(st1, "c", swap)
    out = merge(acc0, st0, racc, rst)
    out = lax.all_to_all(out, ("yh", "yl"), split_axis=0, concat_axis=2, tiled=True)
    return out.reshape(STRIP, H * DH)


def solution(mesh):
    fine = Mesh(mesh.devices.reshape(2, 8, 2, 4, 2), AXES)
    return jax.shard_map(
        per_device,
        mesh=fine,
        in_specs=(P(AXES, None),) * 3,
        out_specs=P(AXES, None),
        check_vma=False,
    )
```

```python
import functools
import math

import jax
import jax.numpy as jnp
from jax import lax
from jax.experimental import pallas as pl
from jax.experimental.pallas import tpu as pltpu
from jax.sharding import Mesh, PartitionSpec as P

H = 32
KV = 4
DH = 128
STRIP = 64
C2 = math.log2(math.e) / math.sqrt(DH)
NEG = -1e30
HALF = 1040
AXES = ("yh", "z", "yl", "x", "c")
VMEM = pl.BlockSpec(memory_space=pltpu.VMEM)
SMEM = pl.BlockSpec(memory_space=pltpu.SMEM)


def prep_kernel(kv_ref, out_ref):
    for half in range(2):
        base = half * HALF
        norm = jnp.zeros((1, 1), jnp.float32)
        for s in range(8):
            k = kv_ref[half * 8 + s, :64, :]
            out_ref[base + s * 64 : base + (s + 1) * 64, :] = k
            kf = k.astype(jnp.float32)
            norm = jnp.maximum(norm, jnp.max(jnp.sum(kf * kf, axis=1, keepdims=True), axis=0, keepdims=True))
        for b in range(4):
            src = half * 8 + 2 * b
            block = jnp.concatenate([kv_ref[src, 64:, :], kv_ref[src + 1, 64:, :]], axis=0)
            at = base + 512 + b * 128
            out_ref[at : at + 128, :] = block.astype(jnp.float32).T.astype(jnp.bfloat16)
        bound = jnp.broadcast_to(jnp.sqrt(norm) * 1.01, (16, DH)).astype(jnp.bfloat16)
        out_ref[base + 1024 : base + HALF, :] = bound


def prep(kv):
    return pl.pallas_call(
        prep_kernel,
        out_shape=jax.ShapeDtypeStruct((2 * HALF, DH), jnp.bfloat16),
        in_specs=[VMEM],
        out_specs=VMEM,
        name="prep",
        compiler_params=pltpu.CompilerParams(vmem_limit_bytes=8 * 1024 * 1024),
        cost_estimate=pl.CostEstimate(flops=1000000, bytes_accessed=1000000, transcendentals=0),
    )(kv)


def rows_of(q_ref, t, hq):
    x = q_ref[t, :, pl.ds(pl.multiple_of(hq * 4 * DH, DH), 4 * DH)]
    return jnp.concatenate([x[:, i * DH : (i + 1) * DH] for i in range(4)], axis=0)


def qk(k_blk, rows):
    return lax.dot_general(k_blk, rows, (((1,), (1,)), ((), ())), preferred_element_type=jnp.float32)


def finish_piece(acc_ref, st_ref, t, hq, vt_blk, s, m_new, mask):
    m_old = st_ref[t, hq, 0:1, :]
    l_old = st_ref[t, hq, 1:2, :]
    p = jnp.exp2(s * C2 - m_new)
    if mask is not None:
        p = jnp.where(mask, p, 0.0)
    alpha = jnp.exp2(m_old - m_new)
    pv = lax.dot_general(
        vt_blk, p.astype(jnp.bfloat16), (((1,), (0,)), ((), ())), preferred_element_type=jnp.float32
    )
    st_ref[t, hq, 0:1, :] = m_new
    st_ref[t, hq, 1:2, :] = alpha * l_old + jnp.sum(p, axis=0, keepdims=True)
    acc_ref[t, hq] = alpha * acc_ref[t, hq] + pv


def unit(refs, ch_ref, half, tp, fast, masks=None):
    q_refs, acc_refs, st_refs = refs
    base = pl.multiple_of(half * HALF, 16)
    k_blk = ch_ref[pl.ds(base, 512), :]
    vt_blk = jnp.concatenate([ch_ref[pl.ds(base + 512 + b * 128, 128), :] for b in range(4)], axis=1)
    kn = ch_ref[pl.ds(base + 1024, 16), :].astype(jnp.float32)[0:1, :]
    kn = jnp.concatenate([kn, kn], axis=1)

    def mask_of(w, i):
        return (None, None) if masks is None else masks(w, i)

    if fast:
        todo = [(w, i, hq) for i in range(2) for w in range(2) for hq in range(2)]
        ahead = 2
        scores = [qk(k_blk, rows_of(q_refs[w], 2 * tp + i, hq)) for w, i, hq in todo[:ahead]]
        for n, (w, i, hq) in enumerate(todo):
            if n + ahead < len(todo):
                w2, i2, hq2 = todo[n + ahead]
                scores.append(qk(k_blk, rows_of(q_refs[w2], 2 * tp + i2, hq2)))
            t = 2 * tp + i
            mask, some = mask_of(w, i)
            bound = st_refs[w][t, hq, 2:3, :] * kn
            if some is not None:
                bound = jnp.where(some, bound, NEG)
            m_new = jnp.maximum(st_refs[w][t, hq, 0:1, :], bound)
            finish_piece(acc_refs[w], st_refs[w], t, hq, vt_blk, scores[n], m_new, mask)
        return
    for w in range(2):

        def body(n, carry, w=w):
            i, hq = n // 2, n % 2
            t = 2 * tp + i
            mask, _ = mask_of(w, i)
            s = qk(k_blk, rows_of(q_refs[w], t, hq))
            if mask is not None:
                s = jnp.where(mask, s, NEG)
            top = jnp.maximum(jnp.max(s, axis=0, keepdims=True) * C2, NEG)
            m_new = jnp.maximum(st_refs[w][t, hq, 0:1, :], top)
            finish_piece(acc_refs[w], st_refs[w], t, hq, vt_blk, s, m_new, mask)
            return carry

        lax.fori_loop(0, 4, body, 0)


def both_ways(fast, run):
    @pl.when(fast)
    def _():
        run(True)

    @pl.when(jnp.logical_not(fast))
    def _():
        run(False)


def is_fast(st_ref, ch_ref, halves):
    kn = functools.reduce(
        jnp.maximum, [ch_ref[h * HALF + 1024 : h * HALF + 1040, :].astype(jnp.float32) for h in range(halves)]
    )
    return jnp.max(kn[0:1, :] * st_ref[0, 0, 3:4, 0:DH]) <= 60.0


def own_kernel(sc_ref, q0, q1, ch_ref, acc0, acc1, st0, st1):
    x, c = sc_ref[1], sc_ref[2]
    refs = ((q0, q1), (acc0, acc1), (st0, st1))
    ones = jnp.ones((16, DH), jnp.bfloat16)
    widest = jnp.zeros((1, 256), jnp.float32)
    for w in range(2):
        refs[1][w][...] = jnp.zeros_like(refs[1][w])
        for t in range(4):
            for hq in range(2):
                r = rows_of(refs[0][w], t, hq).astype(jnp.float32)
                n2 = qk(ones, (r * r).astype(jnp.bfloat16))[0:1, :]
                qn = jnp.sqrt(n2) * (1.02 * C2)
                widest = jnp.maximum(widest, qn)
                refs[2][w][t, hq, 0:1, :] = jnp.full((1, 256), NEG, jnp.float32)
                refs[2][w][t, hq, 1:2, :] = jnp.zeros((1, 256), jnp.float32)
                refs[2][w][t, hq, 2:3, :] = qn
    st0[0, 0, 3:4, :] = jnp.broadcast_to(jnp.max(widest, axis=1, keepdims=True), (1, 256))

    row = lax.broadcasted_iota(jnp.int32, (1, 256), 1) % STRIP
    key = lax.broadcasted_iota(jnp.int32, (512, 1), 0)
    key_pos = (key // 256) * 512 + ((key % 256) // STRIP) * 128 + c * STRIP + key % STRIP

    def masks(w, i):
        row_pos = i * 512 + x * 128 + (c if w == 0 else 1 - c) * STRIP + row
        return key_pos <= row_pos, c * STRIP <= row_pos

    def run(fast):
        def diagonal(h, carry):
            unit(refs, ch_ref, h, h, fast, masks)
            return carry

        lax.fori_loop(0, 2, diagonal, 0)
        unit(refs, ch_ref, 0, 1, fast)

    both_ways(is_fast(st0, ch_ref, 2), run)


def step_kernel(parts, sc_ref, q0, q1, *refs):
    n = len(parts)
    refs, chunks = ((q0, q1), refs[n + 4 : n + 6], refs[n + 6 : n + 8]), refs[:n]
    for ch_ref, (halves, at) in zip(chunks, parts):
        before = sc_ref[at]

        def run(fast, ch_ref=ch_ref, halves=halves, before=before):
            def body(u, carry):
                if halves == (0, 1):
                    half, tp = jnp.where(u == 1, 1, 0), jnp.where(u == 2, 0, 1)
                elif halves == (0,):
                    half, tp = 0, 1 - u
                else:
                    half, tp = 0, 1
                unit(refs, ch_ref, half, tp, fast)
                return carry

            count = {(0, 1): 1 + 2 * before, (0,): 1 + before, (1,): before}[halves]
            lax.fori_loop(0, count, body, 0)

        both_ways(is_fast(refs[2][0], ch_ref, len(halves)), run)


ST = (
    jax.ShapeDtypeStruct((4, 2, DH, 256), jnp.float32),
    jax.ShapeDtypeStruct((4, 2, DH, 256), jnp.float32),
    jax.ShapeDtypeStruct((4, 2, 8, 256), jnp.float32),
    jax.ShapeDtypeStruct((4, 2, 8, 256), jnp.float32),
)


def cost(units):
    work = units * 8 * 512 * 256
    return pl.CostEstimate(flops=4 * work * DH, bytes_accessed=6000000, transcendentals=work)


def own_step(sc, q0, q1, chunk):
    return pl.pallas_call(
        own_kernel,
        out_shape=ST,
        in_specs=[SMEM, VMEM, VMEM, VMEM],
        out_specs=(VMEM,) * 4,
        name="own",
        compiler_params=pltpu.CompilerParams(vmem_limit_bytes=24 * 1024 * 1024),
        cost_estimate=cost(6),
    )(sc, q0, q1, chunk)


def ring_step(sc, q0, q1, state, chunks, parts):
    n = len(chunks)
    return pl.pallas_call(
        functools.partial(step_kernel, parts),
        out_shape=ST,
        in_specs=[SMEM, VMEM, VMEM] + [VMEM] * (n + 4),
        out_specs=(VMEM,) * 4,
        input_output_aliases={3 + n + i: i for i in range(4)},
        name="ring",
        compiler_params=pltpu.CompilerParams(vmem_limit_bytes=24 * 1024 * 1024),
        cost_estimate=cost(8),
    )(sc, q0, q1, *chunks, *state)


def merge_kernel(a_ref, s_ref, ra_ref, rs_ref, out_ref):
    for t in range(4):
        for hq in range(2):
            m0, l0 = s_ref[t, hq, 0:1, :], s_ref[t, hq, 1:2, :]
            m1, l1 = rs_ref[t, hq, 0:1, :], rs_ref[t, hq, 1:2, :]
            m = jnp.maximum(m0, m1)
            f0, f1 = jnp.exp2(m0 - m), jnp.exp2(m1 - m)
            total = f0 * l0 + f1 * l1
            out = (f0 * a_ref[t, hq] + f1 * ra_ref[t, hq]) / total
            rows = out.T.astype(jnp.bfloat16)
            for i in range(4):
                at = (hq * 4 + i) * DH
                out_ref[t, :, at : at + DH] = rows[i * STRIP : (i + 1) * STRIP, :]


def merge(acc, st, racc, rst):
    return pl.pallas_call(
        merge_kernel,
        out_shape=jax.ShapeDtypeStruct((4, STRIP, 8 * DH), jnp.bfloat16),
        in_specs=[VMEM] * 4,
        out_specs=VMEM,
        name="merge",
        compiler_params=pltpu.CompilerParams(vmem_limit_bytes=12 * 1024 * 1024),
        cost_estimate=pl.CostEstimate(flops=2000000, bytes_accessed=3000000, transcendentals=0),
    )(acc, st, racc, rst)


def per_device(queries, keys, values):
    z, x, c = lax.axis_index("z"), lax.axis_index("x"), lax.axis_index("c")
    k4 = keys.reshape(STRIP, KV, DH).transpose(1, 0, 2)
    v4 = values.reshape(STRIP, KV, DH).transpose(1, 0, 2)
    kv = jnp.concatenate([k4, v4], axis=1)
    kv = jnp.broadcast_to(kv[:, None], (KV, 4, 2 * STRIP, DH)).reshape(16, 2 * STRIP, DH)
    kv = lax.all_to_all(kv, ("yh", "yl", "x"), split_axis=0, concat_axis=0, tiled=True)
    chunk = prep(kv)

    q = queries.reshape(STRIP, KV, 8 * DH)
    q0 = lax.all_to_all(q, ("yh", "yl"), split_axis=1, concat_axis=0, tiled=True)
    q0 = q0.reshape(4, STRIP, 8 * DH)
    swap = [(0, 1), (1, 0)]
    q1 = lax.ppermute(q0, "c", swap)

    nz = lax.axis_size("z")
    up = [(i, (i + 1) % nz) for i in range(nz)]
    down = [(i, (i - 1) % nz) for i in range(nz)]
    fwd, bwd = [chunk], [chunk]
    for k in range(1, 4):
        fwd.append(lax.ppermute(fwd[-1], "z", up))
        bwd.append(lax.ppermute(bwd[-1], "z", down))
    far_l = lax.ppermute(fwd[3][:HALF], "z", up)
    far_h = lax.ppermute(bwd[3][HALF:], "z", down)

    flags = [(z - k >= 0).astype(jnp.int32) for k in range(5)]
    wraps = [(z + k >= nz).astype(jnp.int32) for k in range(5)]
    sc = jnp.stack([z, x, c, *flags[1:], *wraps[1:]]).astype(jnp.int32)

    state = own_step(sc, q0, q1, chunk)
    for k in range(1, 4):
        parts = (((0, 1), 2 + k), ((0, 1), 6 + k))
        state = ring_step(sc, q0, q1, state, (fwd[k], bwd[k]), parts)
    state = ring_step(sc, q0, q1, state, (far_l, far_h), (((0,), 6), ((1,), 6)))
    acc0, acc1, st0, st1 = state
    racc = lax.ppermute(acc1, "c", swap)
    rst = lax.ppermute(st1, "c", swap)
    out = merge(acc0, st0, racc, rst)
    out = lax.all_to_all(out, ("yh", "yl"), split_axis=0, concat_axis=2, tiled=True)
    return out.reshape(STRIP, H * DH)


def solution(mesh):
    fine = Mesh(mesh.devices.reshape(2, 8, 2, 4, 2), AXES)
    return jax.shard_map(
        per_device,
        mesh=fine,
        in_specs=(P(AXES, None),) * 3,
        out_specs=P(AXES, None),
        check_vma=False,
    )
```

```python
import functools
import math

import jax
import jax.numpy as jnp
from jax import lax
from jax.experimental import pallas as pl
from jax.experimental.pallas import tpu as pltpu
from jax.sharding import Mesh, PartitionSpec as P

H = 32
KV = 4
DH = 128
STRIP = 64
C2 = math.log2(math.e) / math.sqrt(DH)
NEG = -1e30
ROW_M, ROW_L, ROW_Q, ROW_W = (slice(DH + i, DH + i + 1) for i in range(4))
HALF = 1040
AXES = ("yh", "z", "yl", "x", "c")
VMEM = pl.BlockSpec(memory_space=pltpu.VMEM)
SMEM = pl.BlockSpec(memory_space=pltpu.SMEM)


def prep_kernel(kv_ref, out_ref):
    for half in range(2):
        base = half * HALF
        norm = jnp.zeros((1, 1), jnp.float32)
        for s in range(8):
            k = kv_ref[half * 8 + s, :64, :]
            out_ref[base + s * 64 : base + (s + 1) * 64, :] = k
            kf = k.astype(jnp.float32)
            norm = jnp.maximum(norm, jnp.max(jnp.sum(kf * kf, axis=1, keepdims=True), axis=0, keepdims=True))
        for b in range(4):
            src = half * 8 + 2 * b
            block = jnp.concatenate([kv_ref[src, 64:, :], kv_ref[src + 1, 64:, :]], axis=0)
            at = base + 512 + b * 128
            out_ref[at : at + 128, :] = block.astype(jnp.float32).T.astype(jnp.bfloat16)
        bound = jnp.broadcast_to(jnp.sqrt(norm) * 1.01, (16, DH)).astype(jnp.bfloat16)
        out_ref[base + 1024 : base + HALF, :] = bound


def prep(kv):
    return pl.pallas_call(
        prep_kernel,
        out_shape=jax.ShapeDtypeStruct((2 * HALF, DH), jnp.bfloat16),
        in_specs=[VMEM],
        out_specs=VMEM,
        name="prep",
        compiler_params=pltpu.CompilerParams(vmem_limit_bytes=8 * 1024 * 1024),
        cost_estimate=pl.CostEstimate(flops=1000000, bytes_accessed=1000000, transcendentals=0),
    )(kv)


def rows_of(q_ref, y, t, hq):
    x = q_ref[jnp.bitwise_and(y - t + 4, 3), :, pl.ds(pl.multiple_of(hq * 4 * DH, DH), 4 * DH)]
    return jnp.concatenate([x[:, i * DH : (i + 1) * DH] for i in range(4)], axis=0)


def qk(k_blk, rows):
    return lax.dot_general(k_blk, rows, (((1,), (1,)), ((), ())), preferred_element_type=jnp.float32)


def finish_piece(st_ref, t, hq, vt_blk, s, m_new, mask):
    m_old = st_ref[t, hq, ROW_M, :]
    l_old = st_ref[t, hq, ROW_L, :]
    p = jnp.exp2(s * C2 - m_new)
    if mask is not None:
        p = jnp.where(mask, p, 0.0)
    alpha = jnp.exp2(m_old - m_new)
    pv = lax.dot_general(
        vt_blk, p.astype(jnp.bfloat16), (((1,), (0,)), ((), ())), preferred_element_type=jnp.float32
    )
    st_ref[t, hq, ROW_M, :] = m_new
    st_ref[t, hq, ROW_L, :] = alpha * l_old + jnp.sum(p, axis=0, keepdims=True)
    st_ref[t, hq, 0:DH, :] = alpha * st_ref[t, hq, 0:DH, :] + pv


def unit(refs, ch_ref, half, tp, fast, masks=None):
    q_refs, st_refs, y = refs
    base = pl.multiple_of(half * HALF, 16)
    k_blk = ch_ref[pl.ds(base, 512), :]
    vt_blk = jnp.concatenate([ch_ref[pl.ds(base + 512 + b * 128, 128), :] for b in range(4)], axis=1)
    kn = ch_ref[pl.ds(base + 1024, 16), :].astype(jnp.float32)[0:1, :]
    kn = jnp.concatenate([kn, kn], axis=1)

    def mask_of(w, i):
        return (None, None) if masks is None else masks(w, i)

    if fast:
        todo = [(w, i, hq) for i in range(2) for w in range(2) for hq in range(2)]
        ahead = 2
        scores = [qk(k_blk, rows_of(q_refs[w], y, 2 * tp + i, hq)) for w, i, hq in todo[:ahead]]
        for n, (w, i, hq) in enumerate(todo):
            if n + ahead < len(todo):
                w2, i2, hq2 = todo[n + ahead]
                scores.append(qk(k_blk, rows_of(q_refs[w2], y, 2 * tp + i2, hq2)))
            t = 2 * tp + i
            mask, some = mask_of(w, i)
            bound = st_refs[w][t, hq, ROW_Q, :] * kn
            if some is not None:
                bound = jnp.where(some, bound, NEG)
            m_new = jnp.maximum(st_refs[w][t, hq, ROW_M, :], bound)
            finish_piece(st_refs[w], t, hq, vt_blk, scores[n], m_new, mask)
        return
    for w in range(2):

        def body(n, carry, w=w):
            i, hq = n // 2, n % 2
            t = 2 * tp + i
            mask, _ = mask_of(w, i)
            s = qk(k_blk, rows_of(q_refs[w], y, t, hq))
            if mask is not None:
                s = jnp.where(mask, s, NEG)
            top = jnp.maximum(jnp.max(s, axis=0, keepdims=True) * C2, NEG)
            m_new = jnp.maximum(st_refs[w][t, hq, ROW_M, :], top)
            finish_piece(st_refs[w], t, hq, vt_blk, s, m_new, mask)
            return carry

        lax.fori_loop(0, 4, body, 0)


def both_ways(fast, run):
    @pl.when(fast)
    def _():
        run(True)

    @pl.when(jnp.logical_not(fast))
    def _():
        run(False)


def is_fast(st_ref, chunks):
    kn = functools.reduce(
        jnp.maximum,
        [ch[h * HALF + 1024 : h * HALF + 1040, :].astype(jnp.float32) for ch, halves in chunks for h in range(halves)],
    )
    return jnp.max(kn[0:1, :] * st_ref[0, 0, ROW_W, 0:DH]) <= 60.0


def own_kernel(sc_ref, q0, q1, ch_ref, st0, st1):
    y, x, c = sc_ref[0], sc_ref[1], sc_ref[2]
    refs = ((q0, q1), (st0, st1), y)
    ones = jnp.ones((16, DH), jnp.bfloat16)
    widest = jnp.zeros((1, 256), jnp.float32)
    for q_ref, st_ref in ((q0, st0), (q1, st1)):
        st_ref[:, :, :DH, :] = jnp.zeros((4, 2, DH, 256), jnp.float32)
        for t in range(4):
            for hq in range(2):
                r = rows_of(q_ref, y, t, hq).astype(jnp.float32)
                n2 = qk(ones, (r * r).astype(jnp.bfloat16))[0:1, :]
                qn = jnp.sqrt(n2) * (1.02 * C2)
                widest = jnp.maximum(widest, qn)
                st_ref[t, hq, ROW_M, :] = jnp.full((1, 256), NEG, jnp.float32)
                st_ref[t, hq, ROW_L, :] = jnp.zeros((1, 256), jnp.float32)
                st_ref[t, hq, ROW_Q, :] = qn
    st0[0, 0, ROW_W, :] = jnp.broadcast_to(jnp.max(widest, axis=1, keepdims=True), (1, 256))

    row = lax.broadcasted_iota(jnp.int32, (1, 256), 1) % STRIP
    key = lax.broadcasted_iota(jnp.int32, (512, 1), 0)
    key_pos = (key // 256) * 512 + ((key % 256) // STRIP) * 128 + c * STRIP + key % STRIP

    def masks(w, i):
        row_pos = i * 512 + x * 128 + (c if w == 0 else 1 - c) * STRIP + row
        return key_pos <= row_pos, c * STRIP <= row_pos

    def run(fast):
        def diagonal(h, carry):
            unit(refs, ch_ref, h, h, fast, masks)
            return carry

        lax.fori_loop(0, 2, diagonal, 0)
        unit(refs, ch_ref, 0, 1, fast)

    both_ways(is_fast(st0, [(ch_ref, 2)]), run)


def step_kernel(parts, sc_ref, q0, q1, *refs):
    n = len(parts)
    chunks, refs = refs[:n], ((q0, q1), refs[n + 2 : n + 4], sc_ref[0])

    def run(fast):
        for ch_ref, (halves, at) in zip(chunks, parts):
            before = sc_ref[at]

            def body(u, carry, ch_ref=ch_ref, halves=halves):
                if halves == (0, 1):
                    half, tp = jnp.where(u == 1, 1, 0), jnp.where(u == 2, 0, 1)
                elif halves == (0,):
                    half, tp = 0, 1 - u
                else:
                    half, tp = 0, 1
                unit(refs, ch_ref, half, tp, fast)
                return carry

            count = {(0, 1): 1 + 2 * before, (0,): 1 + before, (1,): before}[halves]
            lax.fori_loop(0, count, body, 0)

    both_ways(is_fast(refs[1][0], [(ch, len(p[0])) for ch, p in zip(chunks, parts)]), run)


ST = (jax.ShapeDtypeStruct((4, 2, DH + 8, 256), jnp.float32),) * 2


def cost(units):
    work = units * 8 * 512 * 256
    return pl.CostEstimate(flops=4 * work * DH, bytes_accessed=6000000, transcendentals=work)


def small(kernel, out_shape, n_in, name, scalars=True):
    outs = jax.tree.map(lambda _: VMEM, out_shape)
    return pl.pallas_call(
        kernel,
        out_shape=out_shape,
        in_specs=[SMEM] * scalars + [VMEM] * n_in,
        out_specs=outs,
        name=name,
        compiler_params=pltpu.CompilerParams(vmem_limit_bytes=12 * 1024 * 1024),
        cost_estimate=pl.CostEstimate(flops=1000000, bytes_accessed=1000000, transcendentals=0),
    )


def own_step(sc, q0, q1, chunk):
    return pl.pallas_call(
        own_kernel,
        out_shape=ST,
        in_specs=[SMEM, VMEM, VMEM, VMEM],
        out_specs=(VMEM,) * 2,
        name="own",
        compiler_params=pltpu.CompilerParams(vmem_limit_bytes=24 * 1024 * 1024),
        cost_estimate=cost(6),
    )(sc, q0, q1, chunk)


def ring_step(sc, q0, q1, state, chunks, parts):
    n = len(chunks)
    return pl.pallas_call(
        functools.partial(step_kernel, parts),
        out_shape=ST,
        in_specs=[SMEM, VMEM, VMEM] + [VMEM] * (n + 2),
        out_specs=(VMEM,) * 2,
        input_output_aliases={3 + n + i: i for i in range(2)},
        name="ring",
        compiler_params=pltpu.CompilerParams(vmem_limit_bytes=24 * 1024 * 1024),
        cost_estimate=cost(8),
    )(sc, q0, q1, *chunks, *state)


def kv_send_kernel(k_ref, v_ref, out_ref):
    for g in range(KV):
        k, v = k_ref[:, g * DH : (g + 1) * DH], v_ref[:, g * DH : (g + 1) * DH]
        for i in range(4):
            out_ref[g * 4 + i, :STRIP, :] = k
            out_ref[g * 4 + i, STRIP:, :] = v


def q_send_kernel(sc_ref, q_ref, *outs):
    for d in range(4):
        to = jnp.bitwise_and(sc_ref[0] + d, 3)
        outs[d][...] = q_ref[:, pl.ds(pl.multiple_of(to * 8 * DH, 8 * DH), 8 * DH)]


def merge_kernel(sc_ref, s_ref, r_ref, *outs):
    for d in range(4):
        t = jnp.bitwise_and(sc_ref[0] + d, 3)
        for hq in range(2):
            m0, l0 = s_ref[t, hq, ROW_M, :], s_ref[t, hq, ROW_L, :]
            m1, l1 = r_ref[t, hq, ROW_M, :], r_ref[t, hq, ROW_L, :]
            m = jnp.maximum(m0, m1)
            f0, f1 = jnp.exp2(m0 - m), jnp.exp2(m1 - m)
            inv = 1.0 / (f0 * l0 + f1 * l1)
            out = (f0 * inv) * s_ref[t, hq, :DH, :] + (f1 * inv) * r_ref[t, hq, :DH, :]
            rows = out.T.astype(jnp.bfloat16)
            for i in range(4):
                at = (hq * 4 + i) * DH
                outs[d][:, at : at + DH] = rows[i * STRIP : (i + 1) * STRIP, :]


def place_kernel(sc_ref, *refs):
    for d in range(4):
        at = jnp.bitwise_and(sc_ref[0] - d + 4, 3)
        refs[4][:, pl.ds(pl.multiple_of(at * 8 * DH, 8 * DH), 8 * DH)] = refs[d][...]


def per_device(queries, keys, values):
    y = lax.axis_index(("yh", "yl"))
    z, x, c = lax.axis_index("z"), lax.axis_index("x"), lax.axis_index("c")
    nz, ny = lax.axis_size("z"), 4
    swap = [(0, 1), (1, 0)]
    up = [(i, (i + 1) % nz) for i in range(nz)]
    down = [(i, (i - 1) % nz) for i in range(nz)]
    flags = [(z - k >= 0).astype(jnp.int32) for k in range(1, 5)]
    wraps = [(z + k >= nz).astype(jnp.int32) for k in range(1, 5)]
    sc = jnp.stack([y, x, c, *flags, *wraps]).astype(jnp.int32)

    def regroup(pieces):
        moved = [
            lax.ppermute(pieces[d], ("yh", "yl"), [(i, (i + d) % ny) for i in range(ny)]) for d in range(1, ny)
        ]
        return [pieces[0], *moved]

    bf16 = jnp.bfloat16
    piece = jax.ShapeDtypeStruct((STRIP, 8 * DH), bf16)
    sent = jax.ShapeDtypeStruct((16, 2 * STRIP, DH), bf16)
    kv = small(kv_send_kernel, sent, 2, "kv_send", False)(keys, values)
    kv = lax.all_to_all(kv, ("yh", "yl", "x"), split_axis=0, concat_axis=0, tiled=True)
    q0 = jnp.stack(regroup(small(q_send_kernel, (piece,) * 4, 1, "q_send")(sc, queries)))
    q1 = lax.ppermute(q0, "c", swap)
    chunk = prep(kv)

    fwd, bwd = [chunk], [chunk]
    for k in range(1, 4):
        fwd.append(lax.ppermute(fwd[-1], "z", up))
        bwd.append(lax.ppermute(bwd[-1], "z", down))
    far_l = lax.ppermute(fwd[3][:HALF], "z", up)
    far_h = lax.ppermute(bwd[3][HALF:], "z", down)

    state = own_step(sc, q0, q1, chunk)
    for k in range(1, 4):
        parts = (((0, 1), 2 + k), ((0, 1), 6 + k))
        state = ring_step(sc, q0, q1, state, (fwd[k], bwd[k]), parts)
    state = ring_step(sc, q0, q1, state, (far_l, far_h), (((0,), 6), ((1,), 6)))
    other = lax.ppermute(state[1], "c", swap)
    pieces = small(merge_kernel, (piece,) * 4, 2, "merge")(sc, state[0], other)
    out = jax.ShapeDtypeStruct((STRIP, H * DH), bf16)
    return small(place_kernel, out, 4, "place")(sc, *regroup(pieces))


def solution(mesh):
    fine = Mesh(mesh.devices.reshape(2, 8, 2, 4, 2), AXES)
    return jax.shard_map(
        per_device,
        mesh=fine,
        in_specs=(P(AXES, None),) * 3,
        out_specs=P(AXES, None),
        check_vma=False,
    )
```

```python
import functools
import math

import jax
import jax.numpy as jnp
from jax import lax
from jax.experimental import pallas as pl
from jax.experimental.pallas import tpu as pltpu
from jax.sharding import Mesh, PartitionSpec as P


H = 32
KV = 4
DH = 128
STRIP = 64
C2 = math.log2(math.e) / math.sqrt(DH)
NEG = -1e30
ROW_M, ROW_L, ROW_Q, ROW_W = (slice(DH + i, DH + i + 1) for i in range(4))
HALF = 1040
AXES = ("yh", "z", "yl", "x", "c")
VMEM = pl.BlockSpec(memory_space=pltpu.VMEM)
SMEM = pl.BlockSpec(memory_space=pltpu.SMEM)


def prep_kernel(kv_ref, out_ref):
    for half in range(2):
        base = half * HALF
        norm = jnp.zeros((1, 1), jnp.float32)
        for s in range(8):
            k = kv_ref[half * 8 + s, :64, :]
            out_ref[base + s * 64 : base + (s + 1) * 64, :] = k
            kf = k.astype(jnp.float32)
            norm = jnp.maximum(norm, jnp.max(jnp.sum(kf * kf, axis=1, keepdims=True), axis=0, keepdims=True))
        for b in range(4):
            src = half * 8 + 2 * b
            block = jnp.concatenate([kv_ref[src, 64:, :], kv_ref[src + 1, 64:, :]], axis=0)
            at = base + 512 + b * 128
            out_ref[at : at + 128, :] = block.astype(jnp.float32).T.astype(jnp.bfloat16)
        bound = jnp.broadcast_to(jnp.sqrt(norm) * 1.01, (16, DH)).astype(jnp.bfloat16)
        out_ref[base + 1024 : base + HALF, :] = bound


def prep(kv):
    return pl.pallas_call(
        prep_kernel,
        out_shape=jax.ShapeDtypeStruct((2 * HALF, DH), jnp.bfloat16),
        in_specs=[VMEM],
        out_specs=VMEM,
        name="prep",
        compiler_params=pltpu.CompilerParams(vmem_limit_bytes=8 * 1024 * 1024),
        cost_estimate=pl.CostEstimate(flops=1000000, bytes_accessed=1000000, transcendentals=0),
    )(kv)


def rows_of(q_ref, y, t, hq):
    x = q_ref[jnp.bitwise_and(y - t + 4, 3), :, pl.ds(pl.multiple_of(hq * 4 * DH, DH), 4 * DH)]
    return jnp.concatenate([x[:, i * DH : (i + 1) * DH] for i in range(4)], axis=0)


def qk(k_blk, rows):
    return lax.dot_general(k_blk, rows, (((1,), (1,)), ((), ())), preferred_element_type=jnp.float32)


def finish_piece(st_ref, t, hq, vt_blk, s, m_new, mask):
    m_old = st_ref[t, hq, ROW_M, :]
    l_old = st_ref[t, hq, ROW_L, :]
    p = jnp.exp2(s * C2 - m_new)
    if mask is not None:
        p = jnp.where(mask, p, 0.0)
    alpha = jnp.exp2(m_old - m_new)
    pv = lax.dot_general(
        vt_blk, p.astype(jnp.bfloat16), (((1,), (0,)), ((), ())), preferred_element_type=jnp.float32
    )
    st_ref[t, hq, ROW_M, :] = m_new
    st_ref[t, hq, ROW_L, :] = alpha * l_old + jnp.sum(p, axis=0, keepdims=True)
    st_ref[t, hq, 0:DH, :] = alpha * st_ref[t, hq, 0:DH, :] + pv


def unit(refs, ch_ref, half, tp, fast, masks=None):
    q_refs, st_refs, y = refs
    base = pl.multiple_of(half * HALF, 16)
    k_blk = ch_ref[pl.ds(base, 512), :]
    vt_blk = jnp.concatenate([ch_ref[pl.ds(base + 512 + b * 128, 128), :] for b in range(4)], axis=1)
    kn = ch_ref[pl.ds(base + 1024, 16), :].astype(jnp.float32)[0:1, :]
    kn = jnp.concatenate([kn, kn], axis=1)

    def mask_of(w, i):
        return (None, None) if masks is None else masks(w, i)

    if fast:
        todo = [(w, i, hq) for i in range(2) for w in range(2) for hq in range(2)]
        ahead = 2
        scores = [qk(k_blk, rows_of(q_refs[w], y, 2 * tp + i, hq)) for w, i, hq in todo[:ahead]]
        for n, (w, i, hq) in enumerate(todo):
            if n + ahead < len(todo):
                w2, i2, hq2 = todo[n + ahead]
                scores.append(qk(k_blk, rows_of(q_refs[w2], y, 2 * tp + i2, hq2)))
            t = 2 * tp + i
            mask, some = mask_of(w, i)
            bound = st_refs[w][t, hq, ROW_Q, :] * kn
            if some is not None:
                bound = jnp.where(some, bound, NEG)
            m_new = jnp.maximum(st_refs[w][t, hq, ROW_M, :], bound)
            finish_piece(st_refs[w], t, hq, vt_blk, scores[n], m_new, mask)
        return
    for w in range(2):

        def body(n, carry, w=w):
            i, hq = n // 2, n % 2
            t = 2 * tp + i
            mask, _ = mask_of(w, i)
            s = qk(k_blk, rows_of(q_refs[w], y, t, hq))
            if mask is not None:
                s = jnp.where(mask, s, NEG)
            top = jnp.maximum(jnp.max(s, axis=0, keepdims=True) * C2, NEG)
            m_new = jnp.maximum(st_refs[w][t, hq, ROW_M, :], top)
            finish_piece(st_refs[w], t, hq, vt_blk, s, m_new, mask)
            return carry

        lax.fori_loop(0, 4, body, 0)


def both_ways(fast, run):
    @pl.when(fast)
    def _():
        run(True)

    @pl.when(jnp.logical_not(fast))
    def _():
        run(False)


def is_fast(st_ref, chunks):
    kn = functools.reduce(
        jnp.maximum,
        [ch[h * HALF + 1024 : h * HALF + 1040, :].astype(jnp.float32) for ch, halves in chunks for h in range(halves)],
    )
    return jnp.max(kn[0:1, :] * st_ref[0, 0, ROW_W, 0:DH]) <= 60.0


def own_kernel(sc_ref, q0, q1, ch_ref, st0, st1):
    y, x, c = sc_ref[0], sc_ref[1], sc_ref[2]
    refs = ((q0, q1), (st0, st1), y)
    ones = jnp.ones((16, DH), jnp.bfloat16)
    widest = jnp.zeros((1, 256), jnp.float32)
    for q_ref, st_ref in ((q0, st0), (q1, st1)):
        st_ref[:, :, :DH, :] = jnp.zeros((4, 2, DH, 256), jnp.float32)
        for t in range(4):
            for hq in range(2):
                r = rows_of(q_ref, y, t, hq).astype(jnp.float32)
                n2 = qk(ones, (r * r).astype(jnp.bfloat16))[0:1, :]
                qn = jnp.sqrt(n2) * (1.02 * C2)
                widest = jnp.maximum(widest, qn)
                st_ref[t, hq, ROW_M, :] = jnp.full((1, 256), NEG, jnp.float32)
                st_ref[t, hq, ROW_L, :] = jnp.zeros((1, 256), jnp.float32)
                st_ref[t, hq, ROW_Q, :] = qn
    st0[0, 0, ROW_W, :] = jnp.broadcast_to(jnp.max(widest, axis=1, keepdims=True), (1, 256))

    row = lax.broadcasted_iota(jnp.int32, (1, 256), 1) % STRIP
    key = lax.broadcasted_iota(jnp.int32, (512, 1), 0)
    key_pos = (key // 256) * 512 + ((key % 256) // STRIP) * 128 + c * STRIP + key % STRIP

    def masks(w, i):
        row_pos = i * 512 + x * 128 + (c if w == 0 else 1 - c) * STRIP + row
        return key_pos <= row_pos, c * STRIP <= row_pos

    def run(fast):
        def diagonal(h, carry):
            unit(refs, ch_ref, h, h, fast, masks)
            return carry

        lax.fori_loop(0, 2, diagonal, 0)
        unit(refs, ch_ref, 0, 1, fast)

    both_ways(is_fast(st0, [(ch_ref, 2)]), run)


def step_kernel(parts, sc_ref, q0, q1, *refs):
    n = len(parts)
    chunks, refs = refs[:n], ((q0, q1), refs[n + 2 : n + 4], sc_ref[0])

    def run(fast):
        for ch_ref, (halves, at) in zip(chunks, parts):
            before = sc_ref[at]

            def body(u, carry, ch_ref=ch_ref, halves=halves):
                if halves == (0, 1):
                    half, tp = jnp.where(u == 1, 1, 0), jnp.where(u == 2, 0, 1)
                elif halves == (0,):
                    half, tp = 0, 1 - u
                else:
                    half, tp = 0, 1
                unit(refs, ch_ref, half, tp, fast)
                return carry

            count = {(0, 1): 1 + 2 * before, (0,): 1 + before, (1,): before}[halves]
            lax.fori_loop(0, count, body, 0)

    both_ways(is_fast(refs[1][0], [(ch, len(p[0])) for ch, p in zip(chunks, parts)]), run)


ST = (jax.ShapeDtypeStruct((4, 2, DH + 8, 256), jnp.float32),) * 2


def cost(units):
    work = units * 8 * 512 * 256
    return pl.CostEstimate(flops=4 * work * DH, bytes_accessed=6000000, transcendentals=work)


def small(kernel, out_shape, n_in, scalars=True):
    outs = jax.tree.map(lambda _: VMEM, out_shape)
    return pl.pallas_call(
        kernel,
        out_shape=out_shape,
        in_specs=[SMEM] * scalars + [VMEM] * n_in,
        out_specs=outs,
        compiler_params=pltpu.CompilerParams(vmem_limit_bytes=12 * 1024 * 1024),
        cost_estimate=pl.CostEstimate(flops=1000000, bytes_accessed=1000000, transcendentals=0),
    )


def own_step(sc, q0, q1, chunk):
    return pl.pallas_call(
        own_kernel,
        out_shape=ST,
        in_specs=[SMEM, VMEM, VMEM, VMEM],
        out_specs=(VMEM,) * 2,
        name="own",
        compiler_params=pltpu.CompilerParams(vmem_limit_bytes=24 * 1024 * 1024),
        cost_estimate=cost(6),
    )(sc, q0, q1, chunk)


def ring_step(sc, q0, q1, state, chunks, parts):
    n = len(chunks)
    return pl.pallas_call(
        functools.partial(step_kernel, parts),
        out_shape=ST,
        in_specs=[SMEM, VMEM, VMEM] + [VMEM] * (n + 2),
        out_specs=(VMEM,) * 2,
        input_output_aliases={3 + n + i: i for i in range(2)},
        name="ring",
        compiler_params=pltpu.CompilerParams(vmem_limit_bytes=24 * 1024 * 1024),
        cost_estimate=cost(8),
    )(sc, q0, q1, *chunks, *state)


def kv_send_kernel(k_ref, v_ref, out_ref):
    for g in range(KV):
        k, v = k_ref[:, g * DH : (g + 1) * DH], v_ref[:, g * DH : (g + 1) * DH]
        for i in range(4):
            out_ref[g * 4 + i, :STRIP, :] = k
            out_ref[g * 4 + i, STRIP:, :] = v


def q_send_kernel(sc_ref, q_ref, *outs):
    for d in range(4):
        to = jnp.bitwise_and(sc_ref[0] + d, 3)
        outs[d][...] = q_ref[:, pl.ds(pl.multiple_of(to * 8 * DH, 8 * DH), 8 * DH)]


def merge_kernel(sc_ref, s_ref, r_ref, *outs):
    for d in range(4):
        t = jnp.bitwise_and(sc_ref[0] + d, 3)
        for hq in range(2):
            m0, l0 = s_ref[t, hq, ROW_M, :], s_ref[t, hq, ROW_L, :]
            m1, l1 = r_ref[t, hq, ROW_M, :], r_ref[t, hq, ROW_L, :]
            m = jnp.maximum(m0, m1)
            f0, f1 = jnp.exp2(m0 - m), jnp.exp2(m1 - m)
            inv = 1.0 / (f0 * l0 + f1 * l1)
            out = (f0 * inv) * s_ref[t, hq, :DH, :] + (f1 * inv) * r_ref[t, hq, :DH, :]
            rows = out.T.astype(jnp.bfloat16)
            for i in range(4):
                at = (hq * 4 + i) * DH
                outs[d][:, at : at + DH] = rows[i * STRIP : (i + 1) * STRIP, :]


def place_kernel(sc_ref, *refs):
    for d in range(4):
        at = jnp.bitwise_and(sc_ref[0] - d + 4, 3)
        refs[4][:, pl.ds(pl.multiple_of(at * 8 * DH, 8 * DH), 8 * DH)] = refs[d][...]


def per_device(queries, keys, values):
    y = lax.axis_index(("yh", "yl"))
    z, x, c = lax.axis_index("z"), lax.axis_index("x"), lax.axis_index("c")
    nz, ny = lax.axis_size("z"), 4
    swap = [(0, 1), (1, 0)]
    up = [(i, (i + 1) % nz) for i in range(nz)]
    down = [(i, (i - 1) % nz) for i in range(nz)]
    flags = [(z - k >= 0).astype(jnp.int32) for k in range(1, 5)]
    wraps = [(z + k >= nz).astype(jnp.int32) for k in range(1, 5)]
    sc = jnp.stack([y, x, c, *flags, *wraps]).astype(jnp.int32)

    def regroup(pieces):
        moved = []
        for d in range(1, ny):
            moved.append(lax.ppermute(pieces[d], ("yh", "yl"), [(i, (i + d) % ny) for i in range(ny)]))
        return [pieces[0], *moved]

    bf16 = jnp.bfloat16
    piece = jax.ShapeDtypeStruct((STRIP, 8 * DH), bf16)
    sent = jax.ShapeDtypeStruct((16, 2 * STRIP, DH), bf16)
    kv = small(kv_send_kernel, sent, 2, False)(keys, values)
    kv = lax.all_to_all(kv, ("yh", "yl", "x"), split_axis=0, concat_axis=0, tiled=True)
    q0 = jnp.stack(regroup(small(q_send_kernel, (piece,) * 4, 1)(sc, queries)))
    q1 = lax.ppermute(q0, "c", swap)
    chunk = prep(kv)

    fwd, bwd = [chunk], [chunk]
    for _ in range(1, 4):
        fwd.append(lax.ppermute(fwd[-1], "z", up))
        bwd.append(lax.ppermute(bwd[-1], "z", down))
    far_l = lax.ppermute(fwd[3][:HALF], "z", up)
    far_h = lax.ppermute(bwd[3][HALF:], "z", down)

    state = own_step(sc, q0, q1, chunk)
    for k in range(1, 4):
        parts = (((0, 1), 2 + k), ((0, 1), 6 + k))
        state = ring_step(sc, q0, q1, state, (fwd[k], bwd[k]), parts)
    state = ring_step(sc, q0, q1, state, (far_l, far_h), (((0,), 6), ((1,), 6)))
    other = lax.ppermute(state[1], "c", swap)
    pieces = small(merge_kernel, (piece,) * 4, 2)(sc, state[0], other)
    out = jax.ShapeDtypeStruct((STRIP, H * DH), bf16)
    return small(place_kernel, out, 4)(sc, *regroup(pieces))


def solution(mesh):
    fine = Mesh(mesh.devices.reshape(2, 8, 2, 4, 2), AXES)
    return jax.shard_map(
        per_device,
        mesh=fine,
        in_specs=(P(AXES, None),) * 3,
        out_specs=P(AXES, None),
        check_vma=False,
    )
```

```python
import functools
import math

import jax
import jax.numpy as jnp
from jax import lax
from jax.experimental import pallas as pl
from jax.experimental.pallas import tpu as pltpu
from jax.sharding import Mesh, PartitionSpec as P


H = 32
KV = 4
DH = 128
STRIP = 64
C2 = math.log2(math.e) / math.sqrt(DH)
NEG = -1e30
ROW_M, ROW_L, ROW_Q, ROW_W = (slice(DH + i, DH + i + 1) for i in range(4))
HALF = 1040
AXES = ("yh", "z", "yl", "x", "c")
VMEM = pl.BlockSpec(memory_space=pltpu.VMEM)
SMEM = pl.BlockSpec(memory_space=pltpu.SMEM)


def prep_kernel(kv_ref, out_ref):
    for half in range(2):
        base = half * HALF
        norm = jnp.zeros((1, 1), jnp.float32)
        for s in range(8):
            k = kv_ref[half * 8 + s, :64, :]
            out_ref[base + s * 64 : base + (s + 1) * 64, :] = k
            kf = k.astype(jnp.float32)
            norm = jnp.maximum(norm, jnp.max(jnp.sum(kf * kf, axis=1, keepdims=True), axis=0, keepdims=True))
        for b in range(4):
            src = half * 8 + 2 * b
            block = jnp.concatenate([kv_ref[src, 64:, :], kv_ref[src + 1, 64:, :]], axis=0)
            at = base + 512 + b * 128
            out_ref[at : at + 128, :] = block.astype(jnp.float32).T.astype(jnp.bfloat16)
        bound = jnp.broadcast_to(jnp.sqrt(norm) * 1.01, (16, DH)).astype(jnp.bfloat16)
        out_ref[base + 1024 : base + HALF, :] = bound


def prep(kv):
    return pl.pallas_call(
        prep_kernel,
        out_shape=jax.ShapeDtypeStruct((2 * HALF, DH), jnp.bfloat16),
        in_specs=[VMEM],
        out_specs=VMEM,
        name="prep",
        compiler_params=pltpu.CompilerParams(vmem_limit_bytes=8 * 1024 * 1024),
        cost_estimate=pl.CostEstimate(flops=1000000, bytes_accessed=1000000, transcendentals=0),
    )(kv)


def rows_of(q_ref, y, t, hq):
    x = q_ref[jnp.bitwise_and(y - t + 4, 3), :, pl.ds(pl.multiple_of(hq * 4 * DH, DH), 4 * DH)]
    return jnp.concatenate([x[:, i * DH : (i + 1) * DH] for i in range(4)], axis=0)


def qk(k_blk, rows):
    return lax.dot_general(k_blk, rows, (((1,), (1,)), ((), ())), preferred_element_type=jnp.float32)


def finish_piece(st_ref, t, hq, vt_blk, s, m_new, mask):
    m_old = st_ref[t, hq, ROW_M, :]
    l_old = st_ref[t, hq, ROW_L, :]
    p = jnp.exp2(s * C2 - m_new)
    if mask is not None:
        p = jnp.where(mask, p, 0.0)
    alpha = jnp.exp2(m_old - m_new)
    pv = lax.dot_general(
        vt_blk, p.astype(jnp.bfloat16), (((1,), (0,)), ((), ())), preferred_element_type=jnp.float32
    )
    st_ref[t, hq, ROW_M, :] = m_new
    st_ref[t, hq, ROW_L, :] = alpha * l_old + jnp.sum(p, axis=0, keepdims=True)
    st_ref[t, hq, 0:DH, :] = alpha * st_ref[t, hq, 0:DH, :] + pv


def unit(refs, ch_ref, half, tp, fast, masks=None):
    q_refs, st_refs, y = refs
    base = pl.multiple_of(half * HALF, 16)
    k_blk = ch_ref[pl.ds(base, 512), :]
    vt_blk = jnp.concatenate([ch_ref[pl.ds(base + 512 + b * 128, 128), :] for b in range(4)], axis=1)
    kn = ch_ref[pl.ds(base + 1024, 16), :].astype(jnp.float32)[0:1, :]
    kn = jnp.concatenate([kn, kn], axis=1)

    def mask_of(w, i):
        return (None, None) if masks is None else masks(w, i)

    if fast:
        todo = [(w, i, hq) for i in range(2) for w in range(2) for hq in range(2)]
        ahead = 2
        scores = [qk(k_blk, rows_of(q_refs[w], y, 2 * tp + i, hq)) for w, i, hq in todo[:ahead]]
        for n, (w, i, hq) in enumerate(todo):
            if n + ahead < len(todo):
                w2, i2, hq2 = todo[n + ahead]
                scores.append(qk(k_blk, rows_of(q_refs[w2], y, 2 * tp + i2, hq2)))
            t = 2 * tp + i
            mask, some = mask_of(w, i)
            bound = st_refs[w][t, hq, ROW_Q, :] * kn
            if some is not None:
                bound = jnp.where(some, bound, NEG)
            m_new = jnp.maximum(st_refs[w][t, hq, ROW_M, :], bound)
            finish_piece(st_refs[w], t, hq, vt_blk, scores[n], m_new, mask)
        return
    for w in range(2):

        def body(n, carry, w=w):
            i, hq = n // 2, n % 2
            t = 2 * tp + i
            mask, _ = mask_of(w, i)
            s = qk(k_blk, rows_of(q_refs[w], y, t, hq))
            if mask is not None:
                s = jnp.where(mask, s, NEG)
            top = jnp.maximum(jnp.max(s, axis=0, keepdims=True) * C2, NEG)
            m_new = jnp.maximum(st_refs[w][t, hq, ROW_M, :], top)
            finish_piece(st_refs[w], t, hq, vt_blk, s, m_new, mask)
            return carry

        lax.fori_loop(0, 4, body, 0)


def both_ways(fast, run):
    @pl.when(fast)
    def _():
        run(True)

    @pl.when(jnp.logical_not(fast))
    def _():
        run(False)


def is_fast(st_ref, chunks):
    kn = functools.reduce(
        jnp.maximum,
        [ch[h * HALF + 1024 : h * HALF + 1040, :].astype(jnp.float32) for ch, halves in chunks for h in range(halves)],
    )
    return jnp.max(kn[0:1, :] * st_ref[0, 0, ROW_W, 0:DH]) <= 60.0


def own_kernel(sc_ref, q0, q1, ch_ref, st0, st1):
    y, x, c = sc_ref[0], sc_ref[1], sc_ref[2]
    refs = ((q0, q1), (st0, st1), y)
    ones = jnp.ones((16, DH), jnp.bfloat16)
    widest = jnp.zeros((1, 256), jnp.float32)
    for q_ref, st_ref in ((q0, st0), (q1, st1)):
        st_ref[:, :, :DH, :] = jnp.zeros((4, 2, DH, 256), jnp.float32)
        for t in range(4):
            for hq in range(2):
                r = rows_of(q_ref, y, t, hq).astype(jnp.float32)
                n2 = qk(ones, (r * r).astype(jnp.bfloat16))[0:1, :]
                qn = jnp.sqrt(n2) * (1.02 * C2)
                widest = jnp.maximum(widest, qn)
                st_ref[t, hq, ROW_M, :] = jnp.full((1, 256), NEG, jnp.float32)
                st_ref[t, hq, ROW_L, :] = jnp.zeros((1, 256), jnp.float32)
                st_ref[t, hq, ROW_Q, :] = qn
    st0[0, 0, ROW_W, :] = jnp.broadcast_to(jnp.max(widest, axis=1, keepdims=True), (1, 256))

    row = lax.broadcasted_iota(jnp.int32, (1, 256), 1) % STRIP
    key = lax.broadcasted_iota(jnp.int32, (512, 1), 0)
    key_pos = (key // 256) * 512 + ((key % 256) // STRIP) * 128 + c * STRIP + key % STRIP

    def masks(w, i):
        row_pos = i * 512 + x * 128 + (c if w == 0 else 1 - c) * STRIP + row
        return key_pos <= row_pos, c * STRIP <= row_pos

    def run(fast):
        def diagonal(h, carry):
            unit(refs, ch_ref, h, h, fast, masks)
            return carry

        lax.fori_loop(0, 2, diagonal, 0)
        unit(refs, ch_ref, 0, 1, fast)

    both_ways(is_fast(st0, [(ch_ref, 2)]), run)


def step_kernel(parts, sc_ref, q0, q1, *refs):
    n = len(parts)
    chunks, refs = refs[:n], ((q0, q1), refs[n + 2 : n + 4], sc_ref[0])

    def run(fast):
        for ch_ref, (halves, at) in zip(chunks, parts):
            before = sc_ref[at]

            def body(u, carry, ch_ref=ch_ref, halves=halves):
                if halves == (0, 1):
                    half, tp = jnp.where(u == 1, 1, 0), jnp.where(u == 2, 0, 1)
                elif halves == (0,):
                    half, tp = 0, 1 - u
                else:
                    half, tp = 0, 1
                unit(refs, ch_ref, half, tp, fast)
                return carry

            count = {(0, 1): 1 + 2 * before, (0,): 1 + before, (1,): before}[halves]
            lax.fori_loop(0, count, body, 0)

    both_ways(is_fast(refs[1][0], [(ch, len(p[0])) for ch, p in zip(chunks, parts)]), run)


ST = (jax.ShapeDtypeStruct((4, 2, DH + 8, 256), jnp.float32),) * 2


def cost(units):
    work = units * 8 * 512 * 256
    return pl.CostEstimate(flops=4 * work * DH, bytes_accessed=6000000, transcendentals=work)


def small(kernel, out_shape, n_in, scalars=True):
    outs = jax.tree.map(lambda _: VMEM, out_shape)
    return pl.pallas_call(
        kernel,
        out_shape=out_shape,
        in_specs=[SMEM] * scalars + [VMEM] * n_in,
        out_specs=outs,
        compiler_params=pltpu.CompilerParams(vmem_limit_bytes=12 * 1024 * 1024),
        cost_estimate=pl.CostEstimate(flops=1000000, bytes_accessed=1000000, transcendentals=0),
    )


def own_step(sc, q0, q1, chunk):
    return pl.pallas_call(
        own_kernel,
        out_shape=ST,
        in_specs=[SMEM, VMEM, VMEM, VMEM],
        out_specs=(VMEM,) * 2,
        name="own",
        compiler_params=pltpu.CompilerParams(vmem_limit_bytes=24 * 1024 * 1024),
        cost_estimate=cost(6),
    )(sc, q0, q1, chunk)


def ring_step(sc, q0, q1, state, chunks, parts):
    n = len(chunks)
    return pl.pallas_call(
        functools.partial(step_kernel, parts),
        out_shape=ST,
        in_specs=[SMEM, VMEM, VMEM] + [VMEM] * (n + 2),
        out_specs=(VMEM,) * 2,
        input_output_aliases={3 + n + i: i for i in range(2)},
        name="ring",
        compiler_params=pltpu.CompilerParams(vmem_limit_bytes=24 * 1024 * 1024),
        cost_estimate=cost(8),
    )(sc, q0, q1, *chunks, *state)


def kv_send_kernel(k_ref, v_ref, out_ref):
    for g in range(KV):
        k, v = k_ref[:, g * DH : (g + 1) * DH], v_ref[:, g * DH : (g + 1) * DH]
        for i in range(4):
            out_ref[g * 4 + i, :STRIP, :] = k
            out_ref[g * 4 + i, STRIP:, :] = v


def q_send_kernel(sc_ref, q_ref, *outs):
    for d in range(4):
        to = jnp.bitwise_and(sc_ref[0] + d, 3)
        outs[d][...] = q_ref[:, pl.ds(pl.multiple_of(to * 8 * DH, 8 * DH), 8 * DH)]


def join_kernel(a_ref, b_ref, c_ref, d_ref, out_ref):
    for d, ref in enumerate((a_ref, b_ref, c_ref, d_ref)):
        out_ref[d] = ref[...]


def merge_kernel(sc_ref, s_ref, r_ref, *outs):
    for d in range(4):
        t = jnp.bitwise_and(sc_ref[0] + d, 3)
        for hq in range(2):
            m0, l0 = s_ref[t, hq, ROW_M, :], s_ref[t, hq, ROW_L, :]
            m1, l1 = r_ref[t, hq, ROW_M, :], r_ref[t, hq, ROW_L, :]
            m = jnp.maximum(m0, m1)
            f0, f1 = jnp.exp2(m0 - m), jnp.exp2(m1 - m)
            inv = 1.0 / (f0 * l0 + f1 * l1)
            out = (f0 * inv) * s_ref[t, hq, :DH, :] + (f1 * inv) * r_ref[t, hq, :DH, :]
            rows = out.T.astype(jnp.bfloat16)
            for i in range(4):
                at = (hq * 4 + i) * DH
                outs[d][:, at : at + DH] = rows[i * STRIP : (i + 1) * STRIP, :]


def place_kernel(sc_ref, *refs):
    for d in range(4):
        at = jnp.bitwise_and(sc_ref[0] - d + 4, 3)
        refs[4][:, pl.ds(pl.multiple_of(at * 8 * DH, 8 * DH), 8 * DH)] = refs[d][...]


def per_device(queries, keys, values):
    y = lax.axis_index(("yh", "yl"))
    z, x, c = lax.axis_index("z"), lax.axis_index("x"), lax.axis_index("c")
    nz, ny = lax.axis_size("z"), 4
    swap = [(0, 1), (1, 0)]
    up = [(i, (i + 1) % nz) for i in range(nz)]
    down = [(i, (i - 1) % nz) for i in range(nz)]
    flags = [(z - k >= 0).astype(jnp.int32) for k in range(1, 5)]
    wraps = [(z + k >= nz).astype(jnp.int32) for k in range(1, 5)]
    sc = jnp.stack([y, x, c, *flags, *wraps]).astype(jnp.int32)

    def regroup(pieces):
        moved = []
        for d in range(1, ny):
            moved.append(lax.ppermute(pieces[d], ("yh", "yl"), [(i, (i + d) % ny) for i in range(ny)]))
        return [pieces[0], *moved]

    bf16 = jnp.bfloat16
    piece = jax.ShapeDtypeStruct((STRIP, 8 * DH), bf16)
    sent = jax.ShapeDtypeStruct((16, 2 * STRIP, DH), bf16)
    kv = small(kv_send_kernel, sent, 2, False)(keys, values)
    kv = lax.all_to_all(kv, ("yh", "yl", "x"), split_axis=0, concat_axis=0, tiled=True)
    q_pieces = regroup(small(q_send_kernel, (piece,) * 4, 1)(sc, queries))
    q0 = small(join_kernel, jax.ShapeDtypeStruct((4, STRIP, 8 * DH), bf16), 4, False)(*q_pieces)
    q1 = lax.ppermute(q0, "c", swap)
    chunk = prep(kv)

    fwd, bwd = [chunk], [chunk]
    for _ in range(1, 4):
        fwd.append(lax.ppermute(fwd[-1], "z", up))
        bwd.append(lax.ppermute(bwd[-1], "z", down))
    far_l = lax.ppermute(fwd[3][:HALF], "z", up)
    far_h = lax.ppermute(bwd[3][HALF:], "z", down)

    state = own_step(sc, q0, q1, chunk)
    for k in range(1, 4):
        parts = (((0, 1), 2 + k), ((0, 1), 6 + k))
        state = ring_step(sc, q0, q1, state, (fwd[k], bwd[k]), parts)
    state = ring_step(sc, q0, q1, state, (far_l, far_h), (((0,), 6), ((1,), 6)))
    other = lax.ppermute(state[1], "c", swap)
    pieces = small(merge_kernel, (piece,) * 4, 2)(sc, state[0], other)
    out = jax.ShapeDtypeStruct((STRIP, H * DH), bf16)
    return small(place_kernel, out, 4)(sc, *regroup(pieces))


def solution(mesh):
    fine = Mesh(mesh.devices.reshape(2, 8, 2, 4, 2), AXES)
    return jax.shard_map(
        per_device,
        mesh=fine,
        in_specs=(P(AXES, None),) * 3,
        out_specs=P(AXES, None),
        check_vma=False,
    )
```

```python
import functools
import math

import jax
import jax.numpy as jnp
from jax import lax
from jax.experimental import pallas as pl
from jax.experimental.pallas import tpu as pltpu
from jax.sharding import Mesh, PartitionSpec as P


H = 32
KV = 4
DH = 128
STRIP = 64
C2 = math.log2(math.e) / math.sqrt(DH)
NEG = -1e30
ROW_M, ROW_L, ROW_Q, ROW_W = (slice(DH + i, DH + i + 1) for i in range(4))
HALF = 1040
AXES = ("yh", "z", "yl", "x", "c")
VMEM = pl.BlockSpec(memory_space=pltpu.VMEM)
SMEM = pl.BlockSpec(memory_space=pltpu.SMEM)
ANY = pl.BlockSpec(memory_space=pl.ANY)


def prep_kernel(kv_ref, out_ref):
    for half in range(2):
        base = half * HALF
        norm = jnp.zeros((1, 1), jnp.float32)
        for s in range(8):
            k = kv_ref[half * 8 + s, :64, :]
            out_ref[base + s * 64 : base + (s + 1) * 64, :] = k
            kf = k.astype(jnp.float32)
            norm = jnp.maximum(norm, jnp.max(jnp.sum(kf * kf, axis=1, keepdims=True), axis=0, keepdims=True))
        for b in range(4):
            src = half * 8 + 2 * b
            block = jnp.concatenate([kv_ref[src, 64:, :], kv_ref[src + 1, 64:, :]], axis=0)
            at = base + 512 + b * 128
            out_ref[at : at + 128, :] = block.astype(jnp.float32).T.astype(jnp.bfloat16)
        bound = jnp.broadcast_to(jnp.sqrt(norm) * 1.01, (16, DH)).astype(jnp.bfloat16)
        out_ref[base + 1024 : base + HALF, :] = bound


def prep(kv):
    return pl.pallas_call(
        prep_kernel,
        out_shape=jax.ShapeDtypeStruct((2 * HALF, DH), jnp.bfloat16),
        in_specs=[VMEM],
        out_specs=VMEM,
        name="prep",
        compiler_params=pltpu.CompilerParams(vmem_limit_bytes=8 * 1024 * 1024),
        cost_estimate=pl.CostEstimate(flops=1000000, bytes_accessed=1000000, transcendentals=0),
    )(kv)


def rows_of(q_ref, y, t, hq):
    x = q_ref[jnp.bitwise_and(y - t + 4, 3), :, pl.ds(pl.multiple_of(hq * 4 * DH, DH), 4 * DH)]
    return jnp.concatenate([x[:, i * DH : (i + 1) * DH] for i in range(4)], axis=0)


def qk(k_blk, rows):
    return lax.dot_general(k_blk, rows, (((1,), (1,)), ((), ())), preferred_element_type=jnp.float32)


def finish_piece(st_ref, t, hq, vt_blk, s, m_new, mask):
    m_old = st_ref[t, hq, ROW_M, :]
    l_old = st_ref[t, hq, ROW_L, :]
    p = jnp.exp2(s * C2 - m_new)
    if mask is not None:
        p = jnp.where(mask, p, 0.0)
    alpha = jnp.exp2(m_old - m_new)
    pv = lax.dot_general(
        vt_blk, p.astype(jnp.bfloat16), (((1,), (0,)), ((), ())), preferred_element_type=jnp.float32
    )
    st_ref[t, hq, ROW_M, :] = m_new
    st_ref[t, hq, ROW_L, :] = alpha * l_old + jnp.sum(p, axis=0, keepdims=True)
    st_ref[t, hq, 0:DH, :] = alpha * st_ref[t, hq, 0:DH, :] + pv


def unit(refs, ch_ref, half, tp, fast, masks=None):
    q_refs, st_refs, y = refs
    base = pl.multiple_of(half * HALF, 16)
    k_blk = ch_ref[pl.ds(base, 512), :]
    vt_blk = jnp.concatenate([ch_ref[pl.ds(base + 512 + b * 128, 128), :] for b in range(4)], axis=1)
    kn = ch_ref[pl.ds(base + 1024, 16), :].astype(jnp.float32)[0:1, :]
    kn = jnp.concatenate([kn, kn], axis=1)

    def mask_of(w, i):
        return (None, None) if masks is None else masks(w, i)

    if fast:
        todo = [(w, i, hq) for i in range(2) for w in range(len(q_refs)) for hq in range(2)]
        ahead = 4
        scores = [qk(k_blk, rows_of(q_refs[w], y, 2 * tp + i, hq)) for w, i, hq in todo[:ahead]]
        for n, (w, i, hq) in enumerate(todo):
            if n + ahead < len(todo):
                w2, i2, hq2 = todo[n + ahead]
                scores.append(qk(k_blk, rows_of(q_refs[w2], y, 2 * tp + i2, hq2)))
            t = 2 * tp + i
            mask, some = mask_of(w, i)
            bound = st_refs[w][t, hq, ROW_Q, :] * kn
            if some is not None:
                bound = jnp.where(some, bound, NEG)
            m_new = jnp.maximum(st_refs[w][t, hq, ROW_M, :], bound)
            finish_piece(st_refs[w], t, hq, vt_blk, scores[n], m_new, mask)
        return
    for w in range(len(q_refs)):

        def body(n, carry, w=w):
            i, hq = n // 2, n % 2
            t = 2 * tp + i
            mask, _ = mask_of(w, i)
            s = qk(k_blk, rows_of(q_refs[w], y, t, hq))
            if mask is not None:
                s = jnp.where(mask, s, NEG)
            top = jnp.maximum(jnp.max(s, axis=0, keepdims=True) * C2, NEG)
            m_new = jnp.maximum(st_refs[w][t, hq, ROW_M, :], top)
            finish_piece(st_refs[w], t, hq, vt_blk, s, m_new, mask)
            return carry

        lax.fori_loop(0, 4, body, 0)


def both_ways(fast, run):
    @pl.when(fast)
    def _():
        run(True)

    @pl.when(jnp.logical_not(fast))
    def _():
        run(False)


def is_fast(st_ref, chunks):
    kn = functools.reduce(
        jnp.maximum,
        [ch[h * HALF + 1024 : h * HALF + 1040, :].astype(jnp.float32) for ch, halves in chunks for h in range(halves)],
    )
    return jnp.max(kn[0:1, :] * st_ref[0, 0, ROW_W, 0:DH]) <= 60.0


def own_kernel(sc_ref, q0, q1, ch_ref, st0, st1):
    y, x, c = sc_ref[0], sc_ref[1], sc_ref[2]
    refs = ((q0, q1), (st0, st1), y)
    ones = jnp.ones((16, DH), jnp.bfloat16)
    widest = jnp.zeros((1, 256), jnp.float32)
    for q_ref, st_ref in ((q0, st0), (q1, st1)):
        st_ref[:, :, :DH, :] = jnp.zeros((4, 2, DH, 256), jnp.float32)
        for t in range(4):
            for hq in range(2):
                r = rows_of(q_ref, y, t, hq).astype(jnp.float32)
                n2 = qk(ones, (r * r).astype(jnp.bfloat16))[0:1, :]
                qn = jnp.sqrt(n2) * (1.02 * C2)
                widest = jnp.maximum(widest, qn)
                st_ref[t, hq, ROW_M, :] = jnp.full((1, 256), NEG, jnp.float32)
                st_ref[t, hq, ROW_L, :] = jnp.zeros((1, 256), jnp.float32)
                st_ref[t, hq, ROW_Q, :] = qn
    for st_ref in (st0, st1):
        st_ref[0, 0, ROW_W, :] = jnp.broadcast_to(jnp.max(widest, axis=1, keepdims=True), (1, 256))

    row = lax.broadcasted_iota(jnp.int32, (1, 256), 1) % STRIP
    key = lax.broadcasted_iota(jnp.int32, (512, 1), 0)
    key_pos = (key // 256) * 512 + ((key % 256) // STRIP) * 128 + c * STRIP + key % STRIP

    def masks(w, i):
        row_pos = i * 512 + x * 128 + (c if w == 0 else 1 - c) * STRIP + row
        return key_pos <= row_pos, c * STRIP <= row_pos

    def run(fast):
        def diagonal(h, carry):
            unit(refs, ch_ref, h, h, fast, masks)
            return carry

        lax.fori_loop(0, 2, diagonal, 0)
        unit(refs, ch_ref, 0, 1, fast)

    both_ways(is_fast(st0, [(ch_ref, 2)]), run)


def step_kernel(parts, n_rows, sc_ref, *refs):
    q_refs, refs = refs[:n_rows], refs[n_rows:]
    chunks, refs = refs[: len(parts)], (q_refs, refs[-n_rows:], sc_ref[0])

    def run(fast):
        for ch_ref, (halves, at) in zip(chunks, parts):
            before = sc_ref[at]

            def body(u, carry, ch_ref=ch_ref, halves=halves):
                if halves == (0, 1):
                    half, tp = jnp.where(u == 1, 1, 0), jnp.where(u == 2, 0, 1)
                elif halves == (0,):
                    half, tp = 0, 1 - u
                else:
                    half, tp = 0, 1
                unit(refs, ch_ref, half, tp, fast)
                return carry

            count = {(0, 1): 1 + 2 * before, (0,): 1 + before, (1,): before}[halves]
            lax.fori_loop(0, count, body, 0)

    both_ways(is_fast(refs[1][0], [(ch, len(p[0])) for ch, p in zip(chunks, parts)]), run)


ST = (jax.ShapeDtypeStruct((4, 2, DH + 8, 256), jnp.float32),) * 2


def cost(units):
    work = units * 8 * 512 * 256
    return pl.CostEstimate(flops=4 * work * DH, bytes_accessed=6000000, transcendentals=work)


def small(kernel, out_shape, n_in, scalars=True, in_space=VMEM, out_space=VMEM, scratch=(), limit=12):
    return pl.pallas_call(
        kernel,
        out_shape=out_shape,
        in_specs=[SMEM] * scalars + [in_space] * n_in,
        out_specs=jax.tree.map(lambda _: out_space, out_shape),
        scratch_shapes=scratch,
        compiler_params=pltpu.CompilerParams(vmem_limit_bytes=limit * 1024 * 1024),
        cost_estimate=pl.CostEstimate(flops=1000000, bytes_accessed=1000000, transcendentals=0),
    )


def own_step(sc, q0, q1, chunk):
    return pl.pallas_call(
        own_kernel,
        out_shape=ST,
        in_specs=[SMEM, VMEM, VMEM, VMEM],
        out_specs=(VMEM,) * 2,
        name="own",
        compiler_params=pltpu.CompilerParams(vmem_limit_bytes=24 * 1024 * 1024),
        cost_estimate=cost(6),
    )(sc, q0, q1, chunk)


def ring_step(sc, qs, state, chunks, parts):
    n, n_rows = len(chunks), len(qs)
    return pl.pallas_call(
        functools.partial(step_kernel, parts, n_rows),
        out_shape=ST[:n_rows],
        in_specs=[SMEM] + [VMEM] * (n + 2 * n_rows),
        out_specs=(VMEM,) * n_rows,
        input_output_aliases={1 + n_rows + n + i: i for i in range(n_rows)},
        name="ring",
        compiler_params=pltpu.CompilerParams(vmem_limit_bytes=24 * 1024 * 1024),
        cost_estimate=cost(2 * n * n_rows),
    )(sc, *qs, *chunks, *state)


def kv_send_kernel(k_hbm, v_hbm, out_ref, k_ref, v_ref, sems):
    copies = [pltpu.make_async_copy(a, b, sems.at[i]) for i, (a, b) in enumerate(((k_hbm, k_ref), (v_hbm, v_ref)))]
    for copy in copies:
        copy.start()
    for copy in copies:
        copy.wait()
    for g in range(KV):
        k, v = k_ref[:, g * DH : (g + 1) * DH], v_ref[:, g * DH : (g + 1) * DH]
        for i in range(4):
            out_ref[g * 4 + i, :STRIP, :] = k
            out_ref[g * 4 + i, STRIP:, :] = v


def q_send_kernel(sc_ref, q_ref, *outs):
    for d in range(4):
        to = jnp.bitwise_and(sc_ref[0] + d, 3)
        outs[d][...] = q_ref[:, pl.ds(pl.multiple_of(to * 8 * DH, 8 * DH), 8 * DH)]


def join_kernel(a_ref, b_ref, c_ref, d_ref, out_ref):
    for d, ref in enumerate((a_ref, b_ref, c_ref, d_ref)):
        out_ref[d] = ref[...]


def merge_kernel(sc_ref, s_ref, r_ref, *outs):
    for d in range(4):
        t = jnp.bitwise_and(sc_ref[0] + d, 3)
        for hq in range(2):
            m0, l0 = s_ref[t, hq, ROW_M, :], s_ref[t, hq, ROW_L, :]
            m1, l1 = r_ref[t, hq, ROW_M, :], r_ref[t, hq, ROW_L, :]
            m = jnp.maximum(m0, m1)
            f0, f1 = jnp.exp2(m0 - m), jnp.exp2(m1 - m)
            inv = 1.0 / (f0 * l0 + f1 * l1)
            out = (f0 * inv) * s_ref[t, hq, :DH, :] + (f1 * inv) * r_ref[t, hq, :DH, :]
            rows = out.T.astype(jnp.bfloat16)
            for i in range(4):
                at = (hq * 4 + i) * DH
                outs[d][:, at : at + DH] = rows[i * STRIP : (i + 1) * STRIP, :]


def place_kernel(sc_ref, *refs):
    pieces, out_hbm, sems = refs[:4], refs[4], refs[5]
    copies = []
    for d in range(4):
        at = jnp.bitwise_and(sc_ref[0] - d + 4, 3) * (8 * DH)
        columns = pl.ds(pl.multiple_of(at, 8 * DH), 8 * DH)
        copies.append(pltpu.make_async_copy(pieces[d], out_hbm.at[:, columns], sems.at[d]))
    for copy in copies:
        copy.start()
    for copy in copies:
        copy.wait()


def per_device(queries, keys, values):
    y = lax.axis_index(("yh", "yl"))
    z, x, c = lax.axis_index("z"), lax.axis_index("x"), lax.axis_index("c")
    nz, ny = lax.axis_size("z"), 4
    swap = [(0, 1), (1, 0)]
    up = [(i, (i + 1) % nz) for i in range(nz)]
    down = [(i, (i - 1) % nz) for i in range(nz)]
    flags = [(z - k >= 0).astype(jnp.int32) for k in range(1, 5)]
    wraps = [(z + k >= nz).astype(jnp.int32) for k in range(1, 5)]
    sc = jnp.stack([y, x, c, *flags, *wraps]).astype(jnp.int32)

    def regroup(pieces):
        moved = []
        for d in range(1, ny):
            moved.append(lax.ppermute(pieces[d], ("yh", "yl"), [(i, (i + d) % ny) for i in range(ny)]))
        return [pieces[0], *moved]

    bf16 = jnp.bfloat16
    piece = jax.ShapeDtypeStruct((STRIP, 8 * DH), bf16)
    sent = jax.ShapeDtypeStruct((16, 2 * STRIP, DH), bf16)
    held = [pltpu.VMEM((STRIP, KV * DH), bf16)] * 2 + [pltpu.SemaphoreType.DMA((2,))]
    kv = small(kv_send_kernel, sent, 2, False, ANY, VMEM, held, 63)(keys, values)
    kv = lax.all_to_all(kv, ("yh", "yl", "x"), split_axis=0, concat_axis=0, tiled=True)
    q_pieces = regroup(small(q_send_kernel, (piece,) * 4, 1)(sc, queries))
    q0 = small(join_kernel, jax.ShapeDtypeStruct((4, STRIP, 8 * DH), bf16), 4, False)(*q_pieces)
    q1 = lax.ppermute(q0, "c", swap)
    chunk = prep(kv)

    fwd, bwd = [chunk], [chunk]
    for _ in range(1, 4):
        fwd.append(lax.ppermute(fwd[-1], "z", up))
        bwd.append(lax.ppermute(bwd[-1], "z", down))
    far_l = lax.ppermute(fwd[3][:HALF], "z", up)
    far_h = lax.ppermute(bwd[3][HALF:], "z", down)

    state = own_step(sc, q0, q1, chunk)
    for k in range(1, 4):
        parts = (((0, 1), 2 + k), ((0, 1), 6 + k))
        state = ring_step(sc, (q0, q1), state, (fwd[k], bwd[k]), parts)
    far = ((far_l, far_h), (((0,), 6), ((1,), 6)))
    (theirs,) = ring_step(sc, (q1,), state[1:], *far)
    other = lax.ppermute(theirs, "c", swap)
    (ours,) = ring_step(sc, (q0,), state[:1], *far)
    pieces = small(merge_kernel, (piece,) * 4, 2)(sc, ours, other)
    out = jax.ShapeDtypeStruct((STRIP, H * DH), bf16)
    sems = [pltpu.SemaphoreType.DMA((4,))]
    return small(place_kernel, out, 4, True, VMEM, ANY, sems)(sc, *regroup(pieces))


def solution(mesh):
    fine = Mesh(mesh.devices.reshape(2, 8, 2, 4, 2), AXES)
    return jax.shard_map(
        per_device,
        mesh=fine,
        in_specs=(P(AXES, None),) * 3,
        out_specs=P(AXES, None),
        check_vma=False,
    )
```

```python
import functools
import math

import jax
import jax.numpy as jnp
from jax import lax
from jax.experimental import pallas as pl
from jax.experimental.pallas import tpu as pltpu
from jax.sharding import Mesh, PartitionSpec as P


H = 32
KV = 4
DH = 128
STRIP = 64
C2 = math.log2(math.e) / math.sqrt(DH)
NEG = -1e30
ROW_M, ROW_L, ROW_Q, ROW_W = (slice(DH + i, DH + i + 1) for i in range(4))
HALF = 1040
AXES = ("yh", "z", "yl", "x", "c")
VMEM = pl.BlockSpec(memory_space=pltpu.VMEM)
SMEM = pl.BlockSpec(memory_space=pltpu.SMEM)
ANY = pl.BlockSpec(memory_space=pl.ANY)


def prep_kernel(kv_ref, out_ref):
    for half in range(2):
        base = half * HALF
        norm = jnp.zeros((1, 1), jnp.float32)
        for s in range(8):
            k = kv_ref[half * 8 + s, :64, :]
            out_ref[base + s * 64 : base + (s + 1) * 64, :] = k
            kf = k.astype(jnp.float32)
            norm = jnp.maximum(norm, jnp.max(jnp.sum(kf * kf, axis=1, keepdims=True), axis=0, keepdims=True))
        for b in range(4):
            src = half * 8 + 2 * b
            block = jnp.concatenate([kv_ref[src, 64:, :], kv_ref[src + 1, 64:, :]], axis=0)
            at = base + 512 + b * 128
            out_ref[at : at + 128, :] = block.astype(jnp.float32).T.astype(jnp.bfloat16)
        bound = jnp.broadcast_to(jnp.sqrt(norm) * 1.01, (16, DH)).astype(jnp.bfloat16)
        out_ref[base + 1024 : base + HALF, :] = bound


def prep(kv):
    return pl.pallas_call(
        prep_kernel,
        out_shape=jax.ShapeDtypeStruct((2 * HALF, DH), jnp.bfloat16),
        in_specs=[VMEM],
        out_specs=VMEM,
        name="prep",
        compiler_params=pltpu.CompilerParams(vmem_limit_bytes=8 * 1024 * 1024),
        cost_estimate=pl.CostEstimate(flops=1000000, bytes_accessed=1000000, transcendentals=0),
    )(kv)


def rows_of(q_ref, y, t, hq):
    x = q_ref[jnp.bitwise_and(y - t + 4, 3), :, pl.ds(pl.multiple_of(hq * 4 * DH, DH), 4 * DH)]
    return jnp.concatenate([x[:, i * DH : (i + 1) * DH] for i in range(4)], axis=0)


def qk(k_blk, rows):
    return lax.dot_general(k_blk, rows, (((1,), (1,)), ((), ())), preferred_element_type=jnp.float32)


def load_half(get, half):
    base = pl.multiple_of(half * HALF, 16)
    vt_blk = jnp.concatenate([get(base + 512 + b * 128, 128) for b in range(4)], axis=1)
    kn = get(base + 1024, 16).astype(jnp.float32)[0:1, :]
    return get(base, 512), vt_blk, jnp.concatenate([kn, kn], axis=1)


def update(st_ref, t, hq, m_new, m_old, total, pv):
    alpha = jnp.exp2(m_old - m_new)
    st_ref[t, hq, ROW_M, :] = m_new
    st_ref[t, hq, ROW_L, :] = alpha * st_ref[t, hq, ROW_L, :] + total
    st_ref[t, hq, 0:DH, :] = alpha * st_ref[t, hq, 0:DH, :] + pv


def weigh(vt_blk, s, m_new, mask):
    p = jnp.exp2(s * C2 - m_new)
    if mask is not None:
        p = jnp.where(mask, p, 0.0)
    pv = lax.dot_general(
        vt_blk, p.astype(jnp.bfloat16), (((1,), (0,)), ((), ())), preferred_element_type=jnp.float32
    )
    return jnp.sum(p, axis=0, keepdims=True), pv


def fast_unit(refs, get, halves, tp, masks=None):
    q_refs, st_refs, y = refs
    blocks = [load_half(get, half) for half in halves]
    kn = functools.reduce(jnp.maximum, [b[2] for b in blocks])
    todo = [(w, i, hq) for i in range(2) for w in range(len(q_refs)) for hq in range(2)]
    items = [(p, b) for p in todo for b in range(len(blocks))]
    scores = []

    def issue(n):
        if n < len(items):
            (w, i, hq), b = items[n]
            scores.append(qk(blocks[b][0], rows_of(q_refs[w], y, 2 * tp + i, hq)))

    for n in range(4):
        issue(n)
    for n, (w, i, hq) in enumerate(todo):
        t = 2 * tp + i
        mask, some = (None, None) if masks is None else masks(w, i)
        bound = st_refs[w][t, hq, ROW_Q, :] * kn
        if some is not None:
            bound = jnp.where(some, bound, NEG)
        m_old = st_refs[w][t, hq, ROW_M, :]
        m_new = jnp.maximum(m_old, bound)
        total, pv = None, None
        for b in range(len(blocks)):
            at = n * len(blocks) + b
            issue(at + 4)
            part = weigh(blocks[b][1], scores[at], m_new, mask)
            total, pv = part if b == 0 else (total + part[0], pv + part[1])
        update(st_refs[w], t, hq, m_new, m_old, total, pv)


def slow_unit(refs, get, half, tp, masks=None):
    q_refs, st_refs, y = refs
    k_blk, vt_blk, _ = load_half(get, half)
    for w in range(len(q_refs)):

        def body(n, carry, w=w):
            i, hq = n // 2, n % 2
            t = 2 * tp + i
            mask = None if masks is None else masks(w, i)[0]
            s = qk(k_blk, rows_of(q_refs[w], y, t, hq))
            if mask is not None:
                s = jnp.where(mask, s, NEG)
            m_old = st_refs[w][t, hq, ROW_M, :]
            m_new = jnp.maximum(m_old, jnp.maximum(jnp.max(s, axis=0, keepdims=True) * C2, NEG))
            update(st_refs[w], t, hq, m_new, m_old, *weigh(vt_blk, s, m_new, mask))
            return carry

        lax.fori_loop(0, 4, body, 0)


def both_ways(fast, run):
    @pl.when(fast)
    def _():
        run(True)

    @pl.when(jnp.logical_not(fast))
    def _():
        run(False)


def is_fast(st_ref, gets):
    kn = functools.reduce(
        jnp.maximum, [get(h * HALF + 1024, 16).astype(jnp.float32) for get in gets for h in range(2)]
    )
    return jnp.max(kn[0:1, :] * st_ref[0, 0, ROW_W, 0:DH]) <= 60.0


def own_kernel(sc_ref, q0, q1, ch_ref, st0, st1):
    y, x, c = sc_ref[0], sc_ref[1], sc_ref[2]
    refs = ((q0, q1), (st0, st1), y)
    ones = jnp.ones((16, DH), jnp.bfloat16)
    widest = jnp.zeros((1, 256), jnp.float32)
    for q_ref, st_ref in ((q0, st0), (q1, st1)):
        st_ref[:, :, :DH, :] = jnp.zeros((4, 2, DH, 256), jnp.float32)
        for t in range(4):
            for hq in range(2):
                r = rows_of(q_ref, y, t, hq).astype(jnp.float32)
                n2 = qk(ones, (r * r).astype(jnp.bfloat16))[0:1, :]
                qn = jnp.sqrt(n2) * (1.02 * C2)
                widest = jnp.maximum(widest, qn)
                st_ref[t, hq, ROW_M, :] = jnp.full((1, 256), NEG, jnp.float32)
                st_ref[t, hq, ROW_L, :] = jnp.zeros((1, 256), jnp.float32)
                st_ref[t, hq, ROW_Q, :] = qn
    for st_ref in (st0, st1):
        st_ref[0, 0, ROW_W, :] = jnp.broadcast_to(jnp.max(widest, axis=1, keepdims=True), (1, 256))

    row = lax.broadcasted_iota(jnp.int32, (1, 256), 1) % STRIP
    key = lax.broadcasted_iota(jnp.int32, (512, 1), 0)
    key_pos = (key // 256) * 512 + ((key % 256) // STRIP) * 128 + c * STRIP + key % STRIP

    def masks(w, i):
        row_pos = i * 512 + x * 128 + (c if w == 0 else 1 - c) * STRIP + row
        return key_pos <= row_pos, c * STRIP <= row_pos

    def get(at, n):
        return ch_ref[pl.ds(at, n), :]

    def run(fast):
        def diagonal(h, carry):
            if fast:
                fast_unit(refs, get, (h,), h, masks)
            else:
                slow_unit(refs, get, h, h, masks)
            return carry

        lax.fori_loop(0, 2, diagonal, 0)
        if fast:
            fast_unit(refs, get, (0,), 1)
        else:
            slow_unit(refs, get, 0, 1)

    both_ways(is_fast(st0, [get]), run)


def step_kernel(n_chunks, first, n_rows, sc_ref, *refs):
    q_refs, given, held = refs[:n_rows], refs[n_rows : n_rows + 2], refs[-1]
    refs = (q_refs, refs[-1 - n_rows : -1], sc_ref[0])
    if n_chunks == 2:
        held[0], held[1] = given[0][...], given[1][...]
    else:
        held[0, :HALF, :], held[0, HALF:, :] = given[0][...], given[1][...]

    def chunk(j):
        return lambda at, n: held[j, pl.ds(at, n), :]

    def run(fast):
        def each(j, carry):
            before = sc_ref[first + 4 * j]
            if fast:

                @pl.when(before == 1)
                def _():
                    fast_unit(refs, chunk(j), (0, 1), 1)

                fast_unit(refs, chunk(j), (0,), 1 - before)
            else:

                def body(u, carry):
                    slow_unit(refs, chunk(j), jnp.where(u == 1, 1, 0), jnp.where(u == 2, 0, 1))
                    return carry

                lax.fori_loop(0, 1 + 2 * before, body, 0)
            return carry

        lax.fori_loop(0, n_chunks, each, 0)

    both_ways(is_fast(refs[1][0], [chunk(j) for j in range(n_chunks)]), run)


ST = (jax.ShapeDtypeStruct((4, 2, DH + 8, 256), jnp.float32),) * 2


def cost(units):
    work = units * 8 * 512 * 256
    return pl.CostEstimate(flops=4 * work * DH, bytes_accessed=6000000, transcendentals=work)


def small(kernel, out_shape, n_in, scalars=True, in_space=VMEM, out_space=VMEM, scratch=(), limit=12):
    return pl.pallas_call(
        kernel,
        out_shape=out_shape,
        in_specs=[SMEM] * scalars + [in_space] * n_in,
        out_specs=jax.tree.map(lambda _: out_space, out_shape),
        scratch_shapes=scratch,
        compiler_params=pltpu.CompilerParams(vmem_limit_bytes=limit * 1024 * 1024),
        cost_estimate=pl.CostEstimate(flops=1000000, bytes_accessed=1000000, transcendentals=0),
    )


def own_step(sc, q0, q1, chunk):
    return pl.pallas_call(
        own_kernel,
        out_shape=ST,
        in_specs=[SMEM, VMEM, VMEM, VMEM],
        out_specs=(VMEM,) * 2,
        name="own",
        compiler_params=pltpu.CompilerParams(vmem_limit_bytes=24 * 1024 * 1024),
        cost_estimate=cost(6),
    )(sc, q0, q1, chunk)


def ring_step(sc, qs, state, chunks, n_chunks, first):
    n_rows = len(qs)
    return pl.pallas_call(
        functools.partial(step_kernel, n_chunks, first, n_rows),
        out_shape=ST[:n_rows],
        in_specs=[SMEM] + [VMEM] * (2 + 2 * n_rows),
        out_specs=(VMEM,) * n_rows,
        input_output_aliases={3 + n_rows + i: i for i in range(n_rows)},
        scratch_shapes=[pltpu.VMEM((n_chunks, 2 * HALF, DH), jnp.bfloat16)],
        name="ring",
        compiler_params=pltpu.CompilerParams(vmem_limit_bytes=24 * 1024 * 1024),
        cost_estimate=cost(2 * n_chunks * n_rows),
    )(sc, *qs, *chunks, *state)


def kv_send_kernel(k_hbm, v_hbm, out_ref, k_ref, v_ref, sems):
    copies = [pltpu.make_async_copy(a, b, sems.at[i]) for i, (a, b) in enumerate(((k_hbm, k_ref), (v_hbm, v_ref)))]
    for copy in copies:
        copy.start()
    for copy in copies:
        copy.wait()
    for g in range(KV):
        k, v = k_ref[:, g * DH : (g + 1) * DH], v_ref[:, g * DH : (g + 1) * DH]
        for i in range(4):
            out_ref[g * 4 + i, :STRIP, :] = k
            out_ref[g * 4 + i, STRIP:, :] = v


def q_send_kernel(sc_ref, q_ref, *outs):
    for d in range(4):
        to = jnp.bitwise_and(sc_ref[0] + d, 3)
        outs[d][...] = q_ref[:, pl.ds(pl.multiple_of(to * 8 * DH, 8 * DH), 8 * DH)]


def join_kernel(a_ref, b_ref, c_ref, d_ref, out_ref):
    for d, ref in enumerate((a_ref, b_ref, c_ref, d_ref)):
        out_ref[d] = ref[...]


def merge_kernel(sc_ref, s_ref, r_ref, *outs):
    for d in range(4):
        t = jnp.bitwise_and(sc_ref[0] + d, 3)
        for hq in range(2):
            m0, l0 = s_ref[t, hq, ROW_M, :], s_ref[t, hq, ROW_L, :]
            m1, l1 = r_ref[t, hq, ROW_M, :], r_ref[t, hq, ROW_L, :]
            m = jnp.maximum(m0, m1)
            f0, f1 = jnp.exp2(m0 - m), jnp.exp2(m1 - m)
            inv = 1.0 / (f0 * l0 + f1 * l1)
            out = (f0 * inv) * s_ref[t, hq, :DH, :] + (f1 * inv) * r_ref[t, hq, :DH, :]
            rows = out.T.astype(jnp.bfloat16)
            for i in range(4):
                at = (hq * 4 + i) * DH
                outs[d][:, at : at + DH] = rows[i * STRIP : (i + 1) * STRIP, :]


def place_kernel(sc_ref, *refs):
    pieces, out_hbm, sems = refs[:4], refs[4], refs[5]
    copies = []
    for d in range(4):
        at = jnp.bitwise_and(sc_ref[0] - d + 4, 3) * (8 * DH)
        columns = pl.ds(pl.multiple_of(at, 8 * DH), 8 * DH)
        copies.append(pltpu.make_async_copy(pieces[d], out_hbm.at[:, columns], sems.at[d]))
    for copy in copies:
        copy.start()
    for copy in copies:
        copy.wait()


def per_device(queries, keys, values):
    y = lax.axis_index(("yh", "yl"))
    z, x, c = lax.axis_index("z"), lax.axis_index("x"), lax.axis_index("c")
    nz, ny = lax.axis_size("z"), 4
    swap = [(0, 1), (1, 0)]
    up = [(i, (i + 1) % nz) for i in range(nz)]
    down = [(i, (i - 1) % nz) for i in range(nz)]
    flags = [(z - k >= 0).astype(jnp.int32) for k in range(1, 5)]
    wraps = [(z + k >= nz).astype(jnp.int32) for k in range(1, 5)]
    sc = jnp.stack([y, x, c, *flags, *wraps]).astype(jnp.int32)

    def regroup(pieces):
        moved = []
        for d in range(1, ny):
            moved.append(lax.ppermute(pieces[d], ("yh", "yl"), [(i, (i + d) % ny) for i in range(ny)]))
        return [pieces[0], *moved]

    bf16 = jnp.bfloat16
    piece = jax.ShapeDtypeStruct((STRIP, 8 * DH), bf16)
    sent = jax.ShapeDtypeStruct((16, 2 * STRIP, DH), bf16)
    held = [pltpu.VMEM((STRIP, KV * DH), bf16)] * 2 + [pltpu.SemaphoreType.DMA((2,))]
    kv = small(kv_send_kernel, sent, 2, False, ANY, VMEM, held, 63)(keys, values)
    kv = lax.all_to_all(kv, ("yh", "yl", "x"), split_axis=0, concat_axis=0, tiled=True)
    q_pieces = regroup(small(q_send_kernel, (piece,) * 4, 1)(sc, queries))
    q0 = small(join_kernel, jax.ShapeDtypeStruct((4, STRIP, 8 * DH), bf16), 4, False)(*q_pieces)
    q1 = lax.ppermute(q0, "c", swap)
    chunk = prep(kv)

    fwd, bwd = [chunk], [chunk]
    for _ in range(1, 4):
        fwd.append(lax.ppermute(fwd[-1], "z", up))
        bwd.append(lax.ppermute(bwd[-1], "z", down))
    far_l = lax.ppermute(fwd[3][:HALF], "z", up)
    far_h = lax.ppermute(bwd[3][HALF:], "z", down)

    state = own_step(sc, q0, q1, chunk)
    for k in range(1, 4):
        state = ring_step(sc, (q0, q1), state, (fwd[k], bwd[k]), 2, 2 + k)
    far = ((far_l, far_h), 1, 6)
    (theirs,) = ring_step(sc, (q1,), state[1:], *far)
    other = lax.ppermute(theirs, "c", swap)
    (ours,) = ring_step(sc, (q0,), state[:1], *far)
    pieces = small(merge_kernel, (piece,) * 4, 2)(sc, ours, other)
    out = jax.ShapeDtypeStruct((STRIP, H * DH), bf16)
    sems = [pltpu.SemaphoreType.DMA((4,))]
    return small(place_kernel, out, 4, True, VMEM, ANY, sems)(sc, *regroup(pieces))


def solution(mesh):
    fine = Mesh(mesh.devices.reshape(2, 8, 2, 4, 2), AXES)
    return jax.shard_map(
        per_device,
        mesh=fine,
        in_specs=(P(AXES, None),) * 3,
        out_specs=P(AXES, None),
        check_vma=False,
    )
```

```python
import functools
import math

import jax
import jax.numpy as jnp
from jax import lax
from jax.experimental import pallas as pl
from jax.experimental.pallas import tpu as pltpu
from jax.sharding import Mesh, PartitionSpec as P


H = 32
KV = 4
DH = 128
STRIP = 64
C2 = math.log2(math.e) / math.sqrt(DH)
NEG = -1e30
ROW_M, ROW_L, ROW_Q, ROW_W = (slice(DH + i, DH + i + 1) for i in range(4))
HALF = 1040
AXES = ("yh", "z", "yl", "x", "c")
VMEM = pl.BlockSpec(memory_space=pltpu.VMEM)
SMEM = pl.BlockSpec(memory_space=pltpu.SMEM)
ANY = pl.BlockSpec(memory_space=pl.ANY)


def prep_kernel(kv_ref, out_ref):
    for half in range(2):
        base = half * HALF
        norm = jnp.zeros((1, 1), jnp.float32)
        for s in range(8):
            k = kv_ref[half * 8 + s, :64, :]
            out_ref[base + s * 64 : base + (s + 1) * 64, :] = k
            kf = k.astype(jnp.float32)
            norm = jnp.maximum(norm, jnp.max(jnp.sum(kf * kf, axis=1, keepdims=True), axis=0, keepdims=True))
        for b in range(4):
            src = half * 8 + 2 * b
            block = jnp.concatenate([kv_ref[src, 64:, :], kv_ref[src + 1, 64:, :]], axis=0)
            at = base + 512 + b * 128
            out_ref[at : at + 128, :] = block.astype(jnp.float32).T.astype(jnp.bfloat16)
        bound = jnp.broadcast_to(jnp.sqrt(norm) * 1.01, (16, DH)).astype(jnp.bfloat16)
        out_ref[base + 1024 : base + HALF, :] = bound


def prep(kv):
    return pl.pallas_call(
        prep_kernel,
        out_shape=jax.ShapeDtypeStruct((2 * HALF, DH), jnp.bfloat16),
        in_specs=[VMEM],
        out_specs=VMEM,
        name="prep",
        compiler_params=pltpu.CompilerParams(vmem_limit_bytes=2 * 1024 * 1024),
        cost_estimate=pl.CostEstimate(flops=1000000, bytes_accessed=1000000, transcendentals=0),
    )(kv)


def rows_of(q_ref, y, t, hq):
    x = q_ref[jnp.bitwise_and(y - t + 4, 3), :, pl.ds(pl.multiple_of(hq * 4 * DH, DH), 4 * DH)]
    return jnp.concatenate([x[:, i * DH : (i + 1) * DH] for i in range(4)], axis=0)


def qk(k_blk, rows):
    return lax.dot_general(k_blk, rows, (((1,), (1,)), ((), ())), preferred_element_type=jnp.float32)


def load_half(get, half):
    base = pl.multiple_of(half * HALF, 16)
    vt_blk = jnp.concatenate([get(base + 512 + b * 128, 128) for b in range(4)], axis=1)
    kn = get(base + 1024, 16).astype(jnp.float32)[0:1, :]
    return get(base, 512), vt_blk, jnp.concatenate([kn, kn], axis=1)


def update(st_ref, t, hq, m_new, m_old, total, pv):
    alpha = jnp.exp2(m_old - m_new)
    st_ref[t, hq, ROW_M, :] = m_new
    st_ref[t, hq, ROW_L, :] = alpha * st_ref[t, hq, ROW_L, :] + total
    st_ref[t, hq, 0:DH, :] = alpha * st_ref[t, hq, 0:DH, :] + pv


def weigh(vt_blk, s, m_new, mask):
    p = jnp.exp2(s * C2 - m_new)
    if mask is not None:
        p = jnp.where(mask, p, 0.0)
    pv = lax.dot_general(
        vt_blk, p.astype(jnp.bfloat16), (((1,), (0,)), ((), ())), preferred_element_type=jnp.float32
    )
    return jnp.sum(p, axis=0, keepdims=True), pv


def fast_unit(refs, get, halves, tp, masks=None):
    q_refs, st_refs, y = refs
    blocks = [load_half(get, half) for half in halves]
    kn = functools.reduce(jnp.maximum, [b[2] for b in blocks])
    todo = [(w, i, hq) for i in range(2) for w in range(len(q_refs)) for hq in range(2)]
    items = [(p, b) for p in todo for b in range(len(blocks))]
    scores = []

    def issue(n):
        if n < len(items):
            (w, i, hq), b = items[n]
            scores.append(qk(blocks[b][0], rows_of(q_refs[w], y, 2 * tp + i, hq)))

    for n in range(4):
        issue(n)
    for n, (w, i, hq) in enumerate(todo):
        t = 2 * tp + i
        mask, some = (None, None) if masks is None else masks(w, i)
        bound = st_refs[w][t, hq, ROW_Q, :] * kn
        if some is not None:
            bound = jnp.where(some, bound, NEG)
        m_old = st_refs[w][t, hq, ROW_M, :]
        m_new = jnp.maximum(m_old, bound)
        total, pv = None, None
        for b in range(len(blocks)):
            at = n * len(blocks) + b
            issue(at + 4)
            part = weigh(blocks[b][1], scores[at], m_new, mask)
            total, pv = part if b == 0 else (total + part[0], pv + part[1])
        update(st_refs[w], t, hq, m_new, m_old, total, pv)


def slow_unit(refs, get, half, tp, masks=None):
    q_refs, st_refs, y = refs
    k_blk, vt_blk, _ = load_half(get, half)
    for w in range(len(q_refs)):

        def body(n, carry, w=w):
            i, hq = n // 2, n % 2
            t = 2 * tp + i
            mask = None if masks is None else masks(w, i)[0]
            s = qk(k_blk, rows_of(q_refs[w], y, t, hq))
            if mask is not None:
                s = jnp.where(mask, s, NEG)
            m_old = st_refs[w][t, hq, ROW_M, :]
            m_new = jnp.maximum(m_old, jnp.maximum(jnp.max(s, axis=0, keepdims=True) * C2, NEG))
            update(st_refs[w], t, hq, m_new, m_old, *weigh(vt_blk, s, m_new, mask))
            return carry

        lax.fori_loop(0, 4, body, 0)


def both_ways(fast, run):
    @pl.when(fast)
    def _():
        run(True)

    @pl.when(jnp.logical_not(fast))
    def _():
        run(False)


def is_fast(st_ref, gets):
    kn = functools.reduce(
        jnp.maximum, [get(h * HALF + 1024, 16).astype(jnp.float32) for get in gets for h in range(2)]
    )
    return jnp.max(kn[0:1, :] * st_ref[0, 0, ROW_W, 0:DH]) <= 60.0


def own_kernel(sc_ref, q0, q1, ch_ref, st0, st1):
    y, x, c = sc_ref[0], sc_ref[1], sc_ref[2]
    refs = ((q0, q1), (st0, st1), y)
    ones = jnp.ones((16, DH), jnp.bfloat16)
    widest = jnp.zeros((1, 256), jnp.float32)
    for q_ref, st_ref in ((q0, st0), (q1, st1)):
        st_ref[:, :, :DH, :] = jnp.zeros((4, 2, DH, 256), jnp.float32)
        for t in range(4):
            for hq in range(2):
                r = rows_of(q_ref, y, t, hq).astype(jnp.float32)
                n2 = qk(ones, (r * r).astype(jnp.bfloat16))[0:1, :]
                qn = jnp.sqrt(n2) * (1.02 * C2)
                widest = jnp.maximum(widest, qn)
                st_ref[t, hq, ROW_M, :] = jnp.full((1, 256), NEG, jnp.float32)
                st_ref[t, hq, ROW_L, :] = jnp.zeros((1, 256), jnp.float32)
                st_ref[t, hq, ROW_Q, :] = qn
    for st_ref in (st0, st1):
        st_ref[0, 0, ROW_W, :] = jnp.broadcast_to(jnp.max(widest, axis=1, keepdims=True), (1, 256))

    row = lax.broadcasted_iota(jnp.int32, (1, 256), 1) % STRIP
    key = lax.broadcasted_iota(jnp.int32, (512, 1), 0)
    key_pos = (key // 256) * 512 + ((key % 256) // STRIP) * 128 + c * STRIP + key % STRIP

    def masks(w, i):
        row_pos = i * 512 + x * 128 + (c if w == 0 else 1 - c) * STRIP + row
        return key_pos <= row_pos, c * STRIP <= row_pos

    def get(at, n):
        return ch_ref[pl.ds(at, n), :]

    def run(fast):
        def diagonal(h, carry):
            if fast:
                fast_unit(refs, get, (h,), h, masks)
            else:
                slow_unit(refs, get, h, h, masks)
            return carry

        lax.fori_loop(0, 2, diagonal, 0)
        if fast:
            fast_unit(refs, get, (0,), 1)
        else:
            slow_unit(refs, get, 0, 1)

    both_ways(is_fast(st0, [get]), run)


def step_kernel(n_chunks, first, n_rows, sc_ref, *refs):
    q_refs, given, held = refs[:n_rows], refs[n_rows : n_rows + n_chunks], refs[-1]
    refs = (q_refs, refs[-1 - n_rows : -1], sc_ref[0])
    for j in range(n_chunks):
        held[j] = given[j][...]

    def chunk(j):
        return lambda at, n: held[j, pl.ds(at, n), :]

    def run(fast):
        def each(j, carry):
            before = sc_ref[first + 4 * j]
            if fast:

                @pl.when(before == 1)
                def _():
                    fast_unit(refs, chunk(j), (0, 1), 1)

                fast_unit(refs, chunk(j), (0,), 1 - before)
            else:

                def body(u, carry):
                    slow_unit(refs, chunk(j), jnp.where(u == 1, 1, 0), jnp.where(u == 2, 0, 1))
                    return carry

                lax.fori_loop(0, 1 + 2 * before, body, 0)
            return carry

        lax.fori_loop(0, n_chunks, each, 0)

    both_ways(is_fast(refs[1][0], [chunk(j) for j in range(n_chunks)]), run)


ST = (jax.ShapeDtypeStruct((4, 2, DH + 8, 256), jnp.float32),) * 2


def cost(units):
    work = units * 8 * 512 * 256
    return pl.CostEstimate(flops=4 * work * DH, bytes_accessed=6000000, transcendentals=work)


def small(kernel, out_shape, n_in, scalars=True, in_space=VMEM, out_space=VMEM, scratch=(), limit=4):
    return pl.pallas_call(
        kernel,
        out_shape=out_shape,
        in_specs=[SMEM] * scalars + [in_space] * n_in,
        out_specs=jax.tree.map(lambda _: out_space, out_shape),
        scratch_shapes=scratch,
        compiler_params=pltpu.CompilerParams(vmem_limit_bytes=limit * 1024 * 1024),
        cost_estimate=pl.CostEstimate(flops=1000000, bytes_accessed=1000000, transcendentals=0),
    )


def own_step(sc, q0, q1, chunk):
    return pl.pallas_call(
        own_kernel,
        out_shape=ST,
        in_specs=[SMEM, VMEM, VMEM, VMEM],
        out_specs=(VMEM,) * 2,
        name="own",
        compiler_params=pltpu.CompilerParams(vmem_limit_bytes=8 * 1024 * 1024),
        cost_estimate=cost(6),
    )(sc, q0, q1, chunk)


def ring_step(sc, qs, state, chunks, first):
    n, n_rows = len(chunks), len(qs)
    return pl.pallas_call(
        functools.partial(step_kernel, n, first, n_rows),
        out_shape=ST[:n_rows],
        in_specs=[SMEM] + [VMEM] * (n + 2 * n_rows),
        out_specs=(VMEM,) * n_rows,
        input_output_aliases={1 + n_rows + n + i: i for i in range(n_rows)},
        scratch_shapes=[pltpu.VMEM((n, 2 * HALF, DH), jnp.bfloat16)],
        name="ring",
        compiler_params=pltpu.CompilerParams(vmem_limit_bytes=8 * 1024 * 1024),
        cost_estimate=cost(2 * n * n_rows),
    )(sc, *qs, *chunks, *state)


def spread(raw_ref, out_ref):
    for g in range(KV):
        block = raw_ref[:, g * DH : (g + 1) * DH]
        for i in range(4):
            out_ref[g * 4 + i] = block


def kv_send_kernel(k_hbm, v_hbm, out_ref, raw_ref, sems):
    copies = [
        pltpu.make_async_copy(a, raw_ref.at[pl.ds(i * STRIP, STRIP)], sems.at[i]) for i, a in enumerate((k_hbm, v_hbm))
    ]
    for copy in copies:
        copy.start()
    for copy in copies:
        copy.wait()
    spread(raw_ref, out_ref)


def q_send_kernel(sc_ref, q_ref, *outs):
    for d in range(4):
        to = jnp.bitwise_and(sc_ref[0] + d, 3)
        outs[d][...] = q_ref[:, pl.ds(pl.multiple_of(to * 8 * DH, 8 * DH), 8 * DH)]


def join_kernel(a_ref, b_ref, c_ref, d_ref, out_ref):
    for d, ref in enumerate((a_ref, b_ref, c_ref, d_ref)):
        out_ref[d] = ref[...]


def merge_kernel(sc_ref, s_ref, r_ref, *outs):
    for d in range(4):
        t = jnp.bitwise_and(sc_ref[0] + d, 3)
        for hq in range(2):
            m0, l0 = s_ref[t, hq, ROW_M, :], s_ref[t, hq, ROW_L, :]
            m1, l1 = r_ref[t, hq, ROW_M, :], r_ref[t, hq, ROW_L, :]
            m = jnp.maximum(m0, m1)
            f0, f1 = jnp.exp2(m0 - m), jnp.exp2(m1 - m)
            inv = 1.0 / (f0 * l0 + f1 * l1)
            out = (f0 * inv) * s_ref[t, hq, :DH, :] + (f1 * inv) * r_ref[t, hq, :DH, :]
            rows = out.T.astype(jnp.bfloat16)
            for i in range(4):
                at = (hq * 4 + i) * DH
                outs[d][:, at : at + DH] = rows[i * STRIP : (i + 1) * STRIP, :]


def place_kernel(sc_ref, *refs):
    pieces, out_hbm, sems = refs[:4], refs[4], refs[5]
    copies = []
    for d in range(4):
        at = jnp.bitwise_and(sc_ref[0] - d + 4, 3) * (8 * DH)
        columns = pl.ds(pl.multiple_of(at, 8 * DH), 8 * DH)
        copies.append(pltpu.make_async_copy(pieces[d], out_hbm.at[:, columns], sems.at[d]))
    for copy in copies:
        copy.start()
    for copy in copies:
        copy.wait()


def per_device(queries, keys, values):
    y = lax.axis_index(("yh", "yl"))
    z, x, c = lax.axis_index("z"), lax.axis_index("x"), lax.axis_index("c")
    nz, ny = lax.axis_size("z"), 4
    swap = [(0, 1), (1, 0)]
    up = [(i, (i + 1) % nz) for i in range(nz)]
    down = [(i, (i - 1) % nz) for i in range(nz)]
    flags = [(z - k >= 0).astype(jnp.int32) for k in range(1, 5)]
    wraps = [(z + k >= nz).astype(jnp.int32) for k in range(1, 5)]
    sc = jnp.stack([y, x, c, *flags, *wraps]).astype(jnp.int32)

    def regroup(pieces):
        moved = []
        for d in range(1, ny):
            moved.append(lax.ppermute(pieces[d], ("yh", "yl"), [(i, (i + d) % ny) for i in range(ny)]))
        return [pieces[0], *moved]

    bf16 = jnp.bfloat16
    piece = jax.ShapeDtypeStruct((STRIP, 8 * DH), bf16)
    sent = jax.ShapeDtypeStruct((16, 2 * STRIP, DH), bf16)
    raw = jax.ShapeDtypeStruct((2 * STRIP, KV * DH), bf16)
    sems = [pltpu.SemaphoreType.DMA((2,))]
    kv, raw = small(kv_send_kernel, (sent, raw), 2, False, ANY, VMEM, sems, 63)(keys, values)
    kv = lax.all_to_all(kv, ("yh", "yl", "x"), split_axis=0, concat_axis=0, tiled=True)
    raw = lax.ppermute(raw, "z", [(i, (i + nz // 2) % nz) for i in range(nz)])
    far = small(spread, sent, 1, False)(raw)
    far = lax.all_to_all(far, ("yh", "yl", "x"), split_axis=0, concat_axis=0, tiled=True)
    far = prep(far)
    q_pieces = regroup(small(q_send_kernel, (piece,) * 4, 1)(sc, queries))
    q0 = small(join_kernel, jax.ShapeDtypeStruct((4, STRIP, 8 * DH), bf16), 4, False)(*q_pieces)
    q1 = lax.ppermute(q0, "c", swap)
    chunk = prep(kv)

    fwd, bwd = [chunk], [chunk]
    for _ in range(1, 4):
        fwd.append(lax.ppermute(fwd[-1], "z", up))
        bwd.append(lax.ppermute(bwd[-1], "z", down))

    state = own_step(sc, q0, q1, chunk)
    for k in range(1, 3):
        state = ring_step(sc, (q0, q1), state, (fwd[k], bwd[k]), 2 + k)
    state = ring_step(sc, (q0, q1), state, (far,), 6)
    (theirs,) = ring_step(sc, (q1,), state[1:], (fwd[3], bwd[3]), 5)
    other = lax.ppermute(theirs, "c", swap)
    (ours,) = ring_step(sc, (q0,), state[:1], (fwd[3], bwd[3]), 5)
    pieces = small(merge_kernel, (piece,) * 4, 2)(sc, ours, other)
    out = jax.ShapeDtypeStruct((STRIP, H * DH), bf16)
    sems = [pltpu.SemaphoreType.DMA((4,))]
    return small(place_kernel, out, 4, True, VMEM, ANY, sems)(sc, *regroup(pieces))


def solution(mesh):
    fine = Mesh(mesh.devices.reshape(2, 8, 2, 4, 2), AXES)
    return jax.shard_map(
        per_device,
        mesh=fine,
        in_specs=(P(AXES, None),) * 3,
        out_specs=P(AXES, None),
        check_vma=False,
    )
```

```python
import functools
import math

import jax
import jax.numpy as jnp
from jax import lax
from jax.experimental import pallas as pl
from jax.experimental.pallas import tpu as pltpu
from jax.sharding import Mesh, PartitionSpec as P


H = 32
KV = 4
DH = 128
STRIP = 64
C2 = math.log2(math.e) / math.sqrt(DH)
NEG = -1e30
ROW_M, ROW_L, ROW_Q, ROW_W = (slice(DH + i, DH + i + 1) for i in range(4))
HALF = 1040
AXES = ("yh", "z", "yl", "x", "c")
VMEM = pl.BlockSpec(memory_space=pltpu.VMEM)
SMEM = pl.BlockSpec(memory_space=pltpu.SMEM)
ANY = pl.BlockSpec(memory_space=pl.ANY)
HBM = pl.BlockSpec(memory_space=pltpu.HBM)


def prep_kernel(kv_ref, out_ref):
    for half in range(2):
        base = half * HALF
        norm = jnp.zeros((1, 1), jnp.float32)
        for s in range(8):
            k = kv_ref[half * 8 + s, :64, :]
            out_ref[base + s * 64 : base + (s + 1) * 64, :] = k
            kf = k.astype(jnp.float32)
            norm = jnp.maximum(norm, jnp.max(jnp.sum(kf * kf, axis=1, keepdims=True), axis=0, keepdims=True))
        for b in range(4):
            src = half * 8 + 2 * b
            block = jnp.concatenate([kv_ref[src, 64:, :], kv_ref[src + 1, 64:, :]], axis=0)
            at = base + 512 + b * 128
            out_ref[at : at + 128, :] = block.astype(jnp.float32).T.astype(jnp.bfloat16)
        bound = jnp.broadcast_to(jnp.sqrt(norm) * 1.01, (16, DH)).astype(jnp.bfloat16)
        out_ref[base + 1024 : base + HALF, :] = bound


def prep_far_kernel(kv_hbm, out_ref, kv_ref, sem):
    copy = pltpu.make_async_copy(kv_hbm, kv_ref, sem)
    copy.start()
    copy.wait()
    prep_kernel(kv_ref, out_ref)


def prep(kv, far=False):
    return pl.pallas_call(
        prep_far_kernel if far else prep_kernel,
        out_shape=jax.ShapeDtypeStruct((2 * HALF, DH), jnp.bfloat16),
        in_specs=[HBM if far else VMEM],
        out_specs=VMEM,
        scratch_shapes=[pltpu.VMEM((16, 2 * STRIP, DH), jnp.bfloat16), pltpu.SemaphoreType.DMA] if far else [],
        name="prep",
        compiler_params=pltpu.CompilerParams(vmem_limit_bytes=3 * 1024 * 1024),
        cost_estimate=pl.CostEstimate(flops=1000000, bytes_accessed=1000000, transcendentals=0),
    )(kv)


def rows_of(q_ref, y, t, hq):
    x = q_ref[jnp.bitwise_and(y - t + 4, 3), :, pl.ds(pl.multiple_of(hq * 4 * DH, DH), 4 * DH)]
    return jnp.concatenate([x[:, i * DH : (i + 1) * DH] for i in range(4)], axis=0)


def qk(k_blk, rows):
    return lax.dot_general(k_blk, rows, (((1,), (1,)), ((), ())), preferred_element_type=jnp.float32)


def load_half(get, half):
    base = pl.multiple_of(half * HALF, 16)
    vt_blk = jnp.concatenate([get(base + 512 + b * 128, 128) for b in range(4)], axis=1)
    kn = get(base + 1024, 16).astype(jnp.float32)[0:1, :]
    return get(base, 512), vt_blk, jnp.concatenate([kn, kn], axis=1)


def update(st_ref, t, hq, m_new, m_old, total, pv):
    alpha = jnp.exp2(m_old - m_new)
    st_ref[t, hq, ROW_M, :] = m_new
    st_ref[t, hq, ROW_L, :] = alpha * st_ref[t, hq, ROW_L, :] + total
    st_ref[t, hq, 0:DH, :] = alpha * st_ref[t, hq, 0:DH, :] + pv


def weigh(vt_blk, s, m_new, mask):
    p = jnp.exp2(s * C2 - m_new)
    if mask is not None:
        p = jnp.where(mask, p, 0.0)
    pv = lax.dot_general(
        vt_blk, p.astype(jnp.bfloat16), (((1,), (0,)), ((), ())), preferred_element_type=jnp.float32
    )
    return jnp.sum(p, axis=0, keepdims=True), pv


def fast_unit(refs, get, halves, tp, masks=None):
    q_refs, st_refs, y = refs
    blocks = [load_half(get, half) for half in halves]
    kn = functools.reduce(jnp.maximum, [b[2] for b in blocks])
    todo = [(w, i, hq) for i in range(2) for w in range(len(q_refs)) for hq in range(2)]
    items = [(p, b) for p in todo for b in range(len(blocks))]
    scores = []

    def issue(n):
        if n < len(items):
            (w, i, hq), b = items[n]
            scores.append(qk(blocks[b][0], rows_of(q_refs[w], y, 2 * tp + i, hq)))

    for n in range(4):
        issue(n)
    for n, (w, i, hq) in enumerate(todo):
        t = 2 * tp + i
        mask, some = (None, None) if masks is None else masks(w, i)
        bound = st_refs[w][t, hq, ROW_Q, :] * kn
        if some is not None:
            bound = jnp.where(some, bound, NEG)
        m_old = st_refs[w][t, hq, ROW_M, :]
        m_new = jnp.maximum(m_old, bound)
        total, pv = None, None
        for b in range(len(blocks)):
            at = n * len(blocks) + b
            issue(at + 4)
            part = weigh(blocks[b][1], scores[at], m_new, mask)
            total, pv = part if b == 0 else (total + part[0], pv + part[1])
        update(st_refs[w], t, hq, m_new, m_old, total, pv)


def slow_unit(refs, get, half, tp, masks=None):
    q_refs, st_refs, y = refs
    k_blk, vt_blk, _ = load_half(get, half)
    for w in range(len(q_refs)):

        def body(n, carry, w=w):
            i, hq = n // 2, n % 2
            t = 2 * tp + i
            mask = None if masks is None else masks(w, i)[0]
            s = qk(k_blk, rows_of(q_refs[w], y, t, hq))
            if mask is not None:
                s = jnp.where(mask, s, NEG)
            m_old = st_refs[w][t, hq, ROW_M, :]
            m_new = jnp.maximum(m_old, jnp.maximum(jnp.max(s, axis=0, keepdims=True) * C2, NEG))
            update(st_refs[w], t, hq, m_new, m_old, *weigh(vt_blk, s, m_new, mask))
            return carry

        lax.fori_loop(0, 4, body, 0)


def both_ways(fast, run):
    @pl.when(fast)
    def _():
        run(True)

    @pl.when(jnp.logical_not(fast))
    def _():
        run(False)


def is_fast(st_ref, gets):
    kn = functools.reduce(
        jnp.maximum, [get(h * HALF + 1024, 16).astype(jnp.float32) for get in gets for h in range(2)]
    )
    return jnp.max(kn[0:1, :] * st_ref[0, 0, ROW_W, 0:DH]) <= 60.0


def own_kernel(sc_ref, q0, q1, ch_ref, st0, st1):
    y, x, c = sc_ref[0], sc_ref[1], sc_ref[2]
    refs = ((q0, q1), (st0, st1), y)
    ones = jnp.ones((16, DH), jnp.bfloat16)
    widest = jnp.zeros((1, 256), jnp.float32)
    for q_ref, st_ref in ((q0, st0), (q1, st1)):
        st_ref[:, :, :DH, :] = jnp.zeros((4, 2, DH, 256), jnp.float32)
        for t in range(4):
            for hq in range(2):
                r = rows_of(q_ref, y, t, hq).astype(jnp.float32)
                n2 = qk(ones, (r * r).astype(jnp.bfloat16))[0:1, :]
                qn = jnp.sqrt(n2) * (1.02 * C2)
                widest = jnp.maximum(widest, qn)
                st_ref[t, hq, ROW_M, :] = jnp.full((1, 256), NEG, jnp.float32)
                st_ref[t, hq, ROW_L, :] = jnp.zeros((1, 256), jnp.float32)
                st_ref[t, hq, ROW_Q, :] = qn
    for st_ref in (st0, st1):
        st_ref[0, 0, ROW_W, :] = jnp.broadcast_to(jnp.max(widest, axis=1, keepdims=True), (1, 256))

    row = lax.broadcasted_iota(jnp.int32, (1, 256), 1) % STRIP
    key = lax.broadcasted_iota(jnp.int32, (512, 1), 0)
    key_pos = (key // 256) * 512 + ((key % 256) // STRIP) * 128 + c * STRIP + key % STRIP

    def masks(w, i):
        row_pos = i * 512 + x * 128 + (c if w == 0 else 1 - c) * STRIP + row
        return key_pos <= row_pos, c * STRIP <= row_pos

    def get(at, n):
        return ch_ref[pl.ds(at, n), :]

    def run(fast):
        def diagonal(h, carry):
            if fast:
                fast_unit(refs, get, (h,), h, masks)
            else:
                slow_unit(refs, get, h, h, masks)
            return carry

        lax.fori_loop(0, 2, diagonal, 0)
        if fast:
            fast_unit(refs, get, (0,), 1)
        else:
            slow_unit(refs, get, 0, 1)

    both_ways(is_fast(st0, [get]), run)


def step_kernel(in_hbm, flags, n_rows, sc_ref, *refs):
    n_chunks = len(in_hbm)
    q_refs, given, held, sems = refs[:n_rows], refs[n_rows : n_rows + n_chunks], refs[-2], refs[-1]
    refs = (q_refs, refs[-2 - n_rows : -2], sc_ref[0])
    copies = [pltpu.make_async_copy(given[j], held.at[j], sems.at[j]) for j in range(n_chunks) if in_hbm[j]]
    for copy in copies:
        copy.start()
    for j in range(n_chunks):
        if not in_hbm[j]:
            held[j] = given[j][...]
    for copy in copies:
        copy.wait()

    def chunk(j):
        return lambda at, n: held[j, pl.ds(at, n), :]

    def run(fast):
        def each(j, carry):
            before = sc_ref[flags[0] + flags[1] * j]
            if fast:

                @pl.when(before == 1)
                def _():
                    fast_unit(refs, chunk(j), (0, 1), 1)

                fast_unit(refs, chunk(j), (0,), 1 - before)
            else:

                def body(u, carry):
                    slow_unit(refs, chunk(j), jnp.where(u == 1, 1, 0), jnp.where(u == 2, 0, 1))
                    return carry

                lax.fori_loop(0, 1 + 2 * before, body, 0)
            return carry

        lax.fori_loop(0, n_chunks, each, 0)

    both_ways(is_fast(refs[1][0], [chunk(j) for j in range(n_chunks)]), run)


ST = (jax.ShapeDtypeStruct((4, 2, DH + 8, 256), jnp.float32),) * 2


def cost(units):
    work = units * 8 * 512 * 256
    return pl.CostEstimate(flops=4 * work * DH, bytes_accessed=6000000, transcendentals=work)


def small(kernel, out_shape, n_in, scalars=True, in_space=VMEM, out_space=VMEM, scratch=(), limit=4):
    return pl.pallas_call(
        kernel,
        out_shape=out_shape,
        in_specs=[SMEM] * scalars + [in_space] * n_in,
        out_specs=jax.tree.map(lambda _: out_space, out_shape),
        scratch_shapes=scratch,
        compiler_params=pltpu.CompilerParams(vmem_limit_bytes=limit * 1024 * 1024),
        cost_estimate=pl.CostEstimate(flops=1000000, bytes_accessed=1000000, transcendentals=0),
    )


def own_step(sc, q0, q1, chunk):
    return pl.pallas_call(
        own_kernel,
        out_shape=ST,
        in_specs=[SMEM, VMEM, VMEM, VMEM],
        out_specs=(VMEM,) * 2,
        name="own",
        compiler_params=pltpu.CompilerParams(vmem_limit_bytes=8 * 1024 * 1024),
        cost_estimate=cost(6),
    )(sc, q0, q1, chunk)


def ring_step(sc, qs, state, chunks, flags, in_hbm):
    n, n_rows = len(chunks), len(qs)
    return pl.pallas_call(
        functools.partial(step_kernel, in_hbm, flags, n_rows),
        out_shape=ST[:n_rows],
        in_specs=[SMEM] + [VMEM] * n_rows + [HBM if h else VMEM for h in in_hbm] + [VMEM] * n_rows,
        out_specs=(VMEM,) * n_rows,
        input_output_aliases={1 + n_rows + n + i: i for i in range(n_rows)},
        scratch_shapes=[pltpu.VMEM((n, 2 * HALF, DH), jnp.bfloat16), pltpu.SemaphoreType.DMA((n,))],
        name="ring",
        compiler_params=pltpu.CompilerParams(vmem_limit_bytes=8 * 1024 * 1024),
        cost_estimate=cost(2 * n * n_rows),
    )(sc, *qs, *chunks, *state)


def spread(raw_ref, out_ref):
    for g in range(KV):
        block = raw_ref[:, g * DH : (g + 1) * DH]
        for i in range(4):
            out_ref[g * 4 + i] = block


def kv_send_kernel(k_hbm, v_hbm, out_ref, raw_ref, sems):
    copies = [
        pltpu.make_async_copy(a, raw_ref.at[pl.ds(i * STRIP, STRIP)], sems.at[i]) for i, a in enumerate((k_hbm, v_hbm))
    ]
    for copy in copies:
        copy.start()
    for copy in copies:
        copy.wait()
    spread(raw_ref, out_ref)


def q_send_kernel(sc_ref, q_ref, *outs):
    for d in range(4):
        to = jnp.bitwise_and(sc_ref[0] + d, 3)
        outs[d][...] = q_ref[:, pl.ds(pl.multiple_of(to * 8 * DH, 8 * DH), 8 * DH)]


def join_kernel(a_ref, b_ref, c_ref, d_ref, out_ref):
    for d, ref in enumerate((a_ref, b_ref, c_ref, d_ref)):
        out_ref[d] = ref[...]


def merge_kernel(sc_ref, s_ref, r_ref, *outs):
    for d in range(4):
        t = jnp.bitwise_and(sc_ref[0] + d, 3)
        for hq in range(2):
            m0, l0 = s_ref[t, hq, ROW_M, :], s_ref[t, hq, ROW_L, :]
            m1, l1 = r_ref[t, hq, ROW_M, :], r_ref[t, hq, ROW_L, :]
            m = jnp.maximum(m0, m1)
            f0, f1 = jnp.exp2(m0 - m), jnp.exp2(m1 - m)
            inv = 1.0 / (f0 * l0 + f1 * l1)
            out = (f0 * inv) * s_ref[t, hq, :DH, :] + (f1 * inv) * r_ref[t, hq, :DH, :]
            rows = out.T.astype(jnp.bfloat16)
            for i in range(4):
                at = (hq * 4 + i) * DH
                outs[d][:, at : at + DH] = rows[i * STRIP : (i + 1) * STRIP, :]


def place_kernel(sc_ref, *refs):
    pieces, out_hbm, sems = refs[:4], refs[4], refs[5]
    copies = []
    for d in range(4):
        at = jnp.bitwise_and(sc_ref[0] - d + 4, 3) * (8 * DH)
        columns = pl.ds(pl.multiple_of(at, 8 * DH), 8 * DH)
        copies.append(pltpu.make_async_copy(pieces[d], out_hbm.at[:, columns], sems.at[d]))
    for copy in copies:
        copy.start()
    for copy in copies:
        copy.wait()


def per_device(queries, keys, values):
    y = lax.axis_index(("yh", "yl"))
    z, x, c = lax.axis_index("z"), lax.axis_index("x"), lax.axis_index("c")
    nz, ny = lax.axis_size("z"), 4
    swap = [(0, 1), (1, 0)]
    up = [(i, (i + 1) % nz) for i in range(nz)]
    down = [(i, (i - 1) % nz) for i in range(nz)]
    flags = [(z - k >= 0).astype(jnp.int32) for k in range(1, 5)]
    wraps = [(z + k >= nz).astype(jnp.int32) for k in range(1, 5)]
    sc = jnp.stack([y, x, c, *flags, *wraps]).astype(jnp.int32)

    def regroup(pieces):
        moved = []
        for d in range(1, ny):
            moved.append(lax.ppermute(pieces[d], ("yh", "yl"), [(i, (i + d) % ny) for i in range(ny)]))
        return [pieces[0], *moved]

    bf16 = jnp.bfloat16
    piece = jax.ShapeDtypeStruct((STRIP, 8 * DH), bf16)
    sent = jax.ShapeDtypeStruct((16, 2 * STRIP, DH), bf16)
    raw = jax.ShapeDtypeStruct((2 * STRIP, KV * DH), bf16)
    sems = [pltpu.SemaphoreType.DMA((2,))]
    kv, raw = small(kv_send_kernel, (sent, raw), 2, False, ANY, VMEM, sems, 63)(keys, values)
    kv = lax.all_to_all(kv, ("yh", "yl", "x"), split_axis=0, concat_axis=0, tiled=True)
    raw = lax.ppermute(raw, "z", [(i, (i + nz // 2) % nz) for i in range(nz)])
    far = small(spread, sent, 1, False)(raw)
    far = lax.all_to_all(far, ("yh", "yl", "x"), split_axis=0, concat_axis=0, tiled=True)
    far = prep(far, True)
    q_pieces = regroup(small(q_send_kernel, (piece,) * 4, 1)(sc, queries))
    q0 = small(join_kernel, jax.ShapeDtypeStruct((4, STRIP, 8 * DH), bf16), 4, False)(*q_pieces)
    q1 = lax.ppermute(q0, "c", swap)
    chunk = prep(kv)

    fwd, bwd = [chunk], [chunk]
    for _ in range(1, 4):
        fwd.append(lax.ppermute(fwd[-1], "z", up))
        bwd.append(lax.ppermute(bwd[-1], "z", down))

    state = own_step(sc, q0, q1, chunk)
    state = ring_step(sc, (q0, q1), state, (fwd[1], bwd[1]), (3, 4), (True, True))
    state = ring_step(sc, (q0, q1), state, (fwd[2], far, bwd[2]), (4, 2), (True, False, True))
    (theirs,) = ring_step(sc, (q1,), state[1:], (fwd[3], bwd[3]), (5, 4), (False, False))
    other = lax.ppermute(theirs, "c", swap)
    (ours,) = ring_step(sc, (q0,), state[:1], (fwd[3], bwd[3]), (5, 4), (False, False))
    pieces = small(merge_kernel, (piece,) * 4, 2)(sc, ours, other)
    out = jax.ShapeDtypeStruct((STRIP, H * DH), bf16)
    sems = [pltpu.SemaphoreType.DMA((4,))]
    return small(place_kernel, out, 4, True, VMEM, ANY, sems)(sc, *regroup(pieces))


def solution(mesh):
    fine = Mesh(mesh.devices.reshape(2, 8, 2, 4, 2), AXES)
    return jax.shard_map(
        per_device,
        mesh=fine,
        in_specs=(P(AXES, None),) * 3,
        out_specs=P(AXES, None),
        check_vma=False,
    )
```

```python
import functools
import math

import jax
import jax.numpy as jnp
from jax import lax
from jax.experimental import pallas as pl
from jax.experimental.pallas import tpu as pltpu
from jax.sharding import Mesh, PartitionSpec as P


H = 32
KV = 4
DH = 128
STRIP = 64
C2 = math.log2(math.e) / math.sqrt(DH)
NEG = -1e30
ROW_M, ROW_L, ROW_Q, ROW_W = (slice(DH + i, DH + i + 1) for i in range(4))
HALF = 1040
AXES = ("yh", "z", "yl", "x", "c")
VMEM = pl.BlockSpec(memory_space=pltpu.VMEM)
SMEM = pl.BlockSpec(memory_space=pltpu.SMEM)
ANY = pl.BlockSpec(memory_space=pl.ANY)


def prep_kernel(kv_ref, out_ref):
    for half in range(2):
        base = half * HALF
        norm = jnp.zeros((1, 1), jnp.float32)
        for s in range(8):
            k = kv_ref[half * 8 + s, :64, :]
            out_ref[base + s * 64 : base + (s + 1) * 64, :] = k
            kf = k.astype(jnp.float32)
            norm = jnp.maximum(norm, jnp.max(jnp.sum(kf * kf, axis=1, keepdims=True), axis=0, keepdims=True))
        for b in range(4):
            src = half * 8 + 2 * b
            block = jnp.concatenate([kv_ref[src, 64:, :], kv_ref[src + 1, 64:, :]], axis=0)
            at = base + 512 + b * 128
            out_ref[at : at + 128, :] = block.astype(jnp.float32).T.astype(jnp.bfloat16)
        bound = jnp.broadcast_to(jnp.sqrt(norm) * 1.01, (16, DH)).astype(jnp.bfloat16)
        out_ref[base + 1024 : base + HALF, :] = bound


def prep(kv):
    return pl.pallas_call(
        prep_kernel,
        out_shape=jax.ShapeDtypeStruct((2 * HALF, DH), jnp.bfloat16),
        in_specs=[VMEM],
        out_specs=VMEM,
        name="prep",
        compiler_params=pltpu.CompilerParams(vmem_limit_bytes=8 * 1024 * 1024),
        cost_estimate=pl.CostEstimate(flops=1000000, bytes_accessed=1000000, transcendentals=0),
    )(kv)


def rows_of(q_ref, y, t, hq):
    x = q_ref[jnp.bitwise_and(y - t + 4, 3), :, pl.ds(pl.multiple_of(hq * 4 * DH, DH), 4 * DH)]
    return jnp.concatenate([x[:, i * DH : (i + 1) * DH] for i in range(4)], axis=0)


def qk(k_blk, rows):
    return lax.dot_general(k_blk, rows, (((1,), (1,)), ((), ())), preferred_element_type=jnp.float32)


def finish_piece(st_ref, t, hq, vt_blk, s, m_new, mask):
    m_old = st_ref[t, hq, ROW_M, :]
    l_old = st_ref[t, hq, ROW_L, :]
    p = jnp.exp2(s * C2 - m_new)
    if mask is not None:
        p = jnp.where(mask, p, 0.0)
    alpha = jnp.exp2(m_old - m_new)
    pv = lax.dot_general(
        vt_blk, p.astype(jnp.bfloat16), (((1,), (0,)), ((), ())), preferred_element_type=jnp.float32
    )
    st_ref[t, hq, ROW_M, :] = m_new
    st_ref[t, hq, ROW_L, :] = alpha * l_old + jnp.sum(p, axis=0, keepdims=True)
    st_ref[t, hq, 0:DH, :] = alpha * st_ref[t, hq, 0:DH, :] + pv


def unit(refs, ch_ref, half, tp, fast, masks=None):
    q_refs, st_refs, y = refs
    base = pl.multiple_of(half * HALF, 16)
    k_blk = ch_ref[pl.ds(base, 512), :]
    vt_blk = jnp.concatenate([ch_ref[pl.ds(base + 512 + b * 128, 128), :] for b in range(4)], axis=1)
    kn = ch_ref[pl.ds(base + 1024, 16), :].astype(jnp.float32)[0:1, :]
    kn = jnp.concatenate([kn, kn], axis=1)

    def mask_of(w, i):
        return (None, None) if masks is None else masks(w, i)

    if fast:
        todo = [(w, i, hq) for i in range(2) for w in range(len(q_refs)) for hq in range(2)]
        ahead = 4
        scores = [qk(k_blk, rows_of(q_refs[w], y, 2 * tp + i, hq)) for w, i, hq in todo[:ahead]]
        for n, (w, i, hq) in enumerate(todo):
            if n + ahead < len(todo):
                w2, i2, hq2 = todo[n + ahead]
                scores.append(qk(k_blk, rows_of(q_refs[w2], y, 2 * tp + i2, hq2)))
            t = 2 * tp + i
            mask, some = mask_of(w, i)
            bound = st_refs[w][t, hq, ROW_Q, :] * kn
            if some is not None:
                bound = jnp.where(some, bound, NEG)
            m_new = jnp.maximum(st_refs[w][t, hq, ROW_M, :], bound)
            finish_piece(st_refs[w], t, hq, vt_blk, scores[n], m_new, mask)
        return
    for w in range(len(q_refs)):

        def body(n, carry, w=w):
            i, hq = n // 2, n % 2
            t = 2 * tp + i
            mask, _ = mask_of(w, i)
            s = qk(k_blk, rows_of(q_refs[w], y, t, hq))
            if mask is not None:
                s = jnp.where(mask, s, NEG)
            top = jnp.maximum(jnp.max(s, axis=0, keepdims=True) * C2, NEG)
            m_new = jnp.maximum(st_refs[w][t, hq, ROW_M, :], top)
            finish_piece(st_refs[w], t, hq, vt_blk, s, m_new, mask)
            return carry

        lax.fori_loop(0, 4, body, 0)


def both_ways(fast, run):
    @pl.when(fast)
    def _():
        run(True)

    @pl.when(jnp.logical_not(fast))
    def _():
        run(False)


def is_fast(st_ref, chunks):
    kn = functools.reduce(
        jnp.maximum,
        [ch[h * HALF + 1024 : h * HALF + 1040, :].astype(jnp.float32) for ch, halves in chunks for h in range(halves)],
    )
    return jnp.max(kn[0:1, :] * st_ref[0, 0, ROW_W, 0:DH]) <= 60.0


def own_kernel(sc_ref, q0, q1, ch_ref, st0, st1):
    y, x, c = sc_ref[0], sc_ref[1], sc_ref[2]
    refs = ((q0, q1), (st0, st1), y)
    ones = jnp.ones((16, DH), jnp.bfloat16)
    widest = jnp.zeros((1, 256), jnp.float32)
    for q_ref, st_ref in ((q0, st0), (q1, st1)):
        st_ref[:, :, :DH, :] = jnp.zeros((4, 2, DH, 256), jnp.float32)
        for t in range(4):
            for hq in range(2):
                r = rows_of(q_ref, y, t, hq).astype(jnp.float32)
                n2 = qk(ones, (r * r).astype(jnp.bfloat16))[0:1, :]
                qn = jnp.sqrt(n2) * (1.02 * C2)
                widest = jnp.maximum(widest, qn)
                st_ref[t, hq, ROW_M, :] = jnp.full((1, 256), NEG, jnp.float32)
                st_ref[t, hq, ROW_L, :] = jnp.zeros((1, 256), jnp.float32)
                st_ref[t, hq, ROW_Q, :] = qn
    for st_ref in (st0, st1):
        st_ref[0, 0, ROW_W, :] = jnp.broadcast_to(jnp.max(widest, axis=1, keepdims=True), (1, 256))

    row = lax.broadcasted_iota(jnp.int32, (1, 256), 1) % STRIP
    key = lax.broadcasted_iota(jnp.int32, (512, 1), 0)
    key_pos = (key // 256) * 512 + ((key % 256) // STRIP) * 128 + c * STRIP + key % STRIP

    def masks(w, i):
        row_pos = i * 512 + x * 128 + (c if w == 0 else 1 - c) * STRIP + row
        return key_pos <= row_pos, c * STRIP <= row_pos

    def run(fast):
        def diagonal(h, carry):
            unit(refs, ch_ref, h, h, fast, masks)
            return carry

        lax.fori_loop(0, 2, diagonal, 0)
        unit(refs, ch_ref, 0, 1, fast)

    both_ways(is_fast(st0, [(ch_ref, 2)]), run)


def step_kernel(parts, n_rows, sc_ref, *refs):
    q_refs, refs = refs[:n_rows], refs[n_rows:]
    chunks, refs = refs[: len(parts)], (q_refs, refs[-n_rows:], sc_ref[0])

    def run(fast):
        for ch_ref, (halves, at) in zip(chunks, parts):
            before = sc_ref[at]

            def body(u, carry, ch_ref=ch_ref, halves=halves):
                if halves == (0, 1):
                    half, tp = jnp.where(u == 1, 1, 0), jnp.where(u == 2, 0, 1)
                elif halves == (0,):
                    half, tp = 0, 1 - u
                else:
                    half, tp = 0, 1
                unit(refs, ch_ref, half, tp, fast)
                return carry

            count = {(0, 1): 1 + 2 * before, (0,): 1 + before, (1,): before}[halves]
            lax.fori_loop(0, count, body, 0)

    both_ways(is_fast(refs[1][0], [(ch, len(p[0])) for ch, p in zip(chunks, parts)]), run)


ST = (jax.ShapeDtypeStruct((4, 2, DH + 8, 256), jnp.float32),) * 2


def cost(units):
    work = units * 8 * 512 * 256
    return pl.CostEstimate(flops=4 * work * DH, bytes_accessed=6000000, transcendentals=work)


def small(kernel, out_shape, n_in, scalars=True, in_space=VMEM, out_space=VMEM, scratch=(), limit=12):
    return pl.pallas_call(
        kernel,
        out_shape=out_shape,
        in_specs=[SMEM] * scalars + [in_space] * n_in,
        out_specs=jax.tree.map(lambda _: out_space, out_shape),
        scratch_shapes=scratch,
        compiler_params=pltpu.CompilerParams(vmem_limit_bytes=limit * 1024 * 1024),
        cost_estimate=pl.CostEstimate(flops=1000000, bytes_accessed=1000000, transcendentals=0),
    )


def own_step(sc, q0, q1, chunk):
    return pl.pallas_call(
        own_kernel,
        out_shape=ST,
        in_specs=[SMEM, VMEM, VMEM, VMEM],
        out_specs=(VMEM,) * 2,
        name="own",
        compiler_params=pltpu.CompilerParams(vmem_limit_bytes=24 * 1024 * 1024),
        cost_estimate=cost(6),
    )(sc, q0, q1, chunk)


def ring_step(sc, qs, state, chunks, parts):
    n, n_rows = len(chunks), len(qs)
    return pl.pallas_call(
        functools.partial(step_kernel, parts, n_rows),
        out_shape=ST[:n_rows],
        in_specs=[SMEM] + [VMEM] * (n + 2 * n_rows),
        out_specs=(VMEM,) * n_rows,
        input_output_aliases={1 + n_rows + n + i: i for i in range(n_rows)},
        name="ring",
        compiler_params=pltpu.CompilerParams(vmem_limit_bytes=24 * 1024 * 1024),
        cost_estimate=cost(2 * n * n_rows),
    )(sc, *qs, *chunks, *state)


def kv_send_kernel(k_hbm, v_hbm, out_ref, k_ref, v_ref, sems):
    copies = [pltpu.make_async_copy(a, b, sems.at[i]) for i, (a, b) in enumerate(((k_hbm, k_ref), (v_hbm, v_ref)))]
    for copy in copies:
        copy.start()
    for copy in copies:
        copy.wait()
    for g in range(KV):
        k, v = k_ref[:, g * DH : (g + 1) * DH], v_ref[:, g * DH : (g + 1) * DH]
        for i in range(4):
            out_ref[g * 4 + i, :STRIP, :] = k
            out_ref[g * 4 + i, STRIP:, :] = v


def q_send_kernel(sc_ref, q_ref, *outs):
    for d in range(4):
        to = jnp.bitwise_and(sc_ref[0] + d, 3)
        outs[d][...] = q_ref[:, pl.ds(pl.multiple_of(to * 8 * DH, 8 * DH), 8 * DH)]


def join_kernel(a_ref, b_ref, c_ref, d_ref, out_ref):
    for d, ref in enumerate((a_ref, b_ref, c_ref, d_ref)):
        out_ref[d] = ref[...]


def merge_kernel(sc_ref, s_ref, r_ref, *outs):
    for d in range(4):
        t = jnp.bitwise_and(sc_ref[0] + d, 3)
        for hq in range(2):
            m0, l0 = s_ref[t, hq, ROW_M, :], s_ref[t, hq, ROW_L, :]
            m1, l1 = r_ref[t, hq, ROW_M, :], r_ref[t, hq, ROW_L, :]
            m = jnp.maximum(m0, m1)
            f0, f1 = jnp.exp2(m0 - m), jnp.exp2(m1 - m)
            inv = 1.0 / (f0 * l0 + f1 * l1)
            out = (f0 * inv) * s_ref[t, hq, :DH, :] + (f1 * inv) * r_ref[t, hq, :DH, :]
            rows = out.T.astype(jnp.bfloat16)
            for i in range(4):
                at = (hq * 4 + i) * DH
                outs[d][:, at : at + DH] = rows[i * STRIP : (i + 1) * STRIP, :]


def place_kernel(sc_ref, *refs):
    pieces, out_hbm, sems = refs[:4], refs[4], refs[5]
    copies = []
    for d in range(4):
        at = jnp.bitwise_and(sc_ref[0] - d + 4, 3) * (8 * DH)
        columns = pl.ds(pl.multiple_of(at, 8 * DH), 8 * DH)
        copies.append(pltpu.make_async_copy(pieces[d], out_hbm.at[:, columns], sems.at[d]))
    for copy in copies:
        copy.start()
    for copy in copies:
        copy.wait()


def per_device(queries, keys, values):
    y = lax.axis_index(("yh", "yl"))
    z, x, c = lax.axis_index("z"), lax.axis_index("x"), lax.axis_index("c")
    nz, ny = lax.axis_size("z"), 4
    swap = [(0, 1), (1, 0)]
    up = [(i, (i + 1) % nz) for i in range(nz)]
    down = [(i, (i - 1) % nz) for i in range(nz)]
    flags = [(z - k >= 0).astype(jnp.int32) for k in range(1, 5)]
    wraps = [(z + k >= nz).astype(jnp.int32) for k in range(1, 5)]
    sc = jnp.stack([y, x, c, *flags, *wraps]).astype(jnp.int32)

    def regroup(pieces):
        moved = {0: pieces[0]}
        for d in (2, 3, 1):
            moved[d] = lax.ppermute(pieces[d], ("yh", "yl"), [(i, (i + d) % ny) for i in range(ny)])
        return [moved[d] for d in range(ny)]

    bf16 = jnp.bfloat16
    piece = jax.ShapeDtypeStruct((STRIP, 8 * DH), bf16)
    sent = jax.ShapeDtypeStruct((16, 2 * STRIP, DH), bf16)
    held = [pltpu.VMEM((STRIP, KV * DH), bf16)] * 2 + [pltpu.SemaphoreType.DMA((2,))]
    kv = small(kv_send_kernel, sent, 2, False, ANY, VMEM, held, 63)(keys, values)
    kv = lax.all_to_all(kv, ("yh", "yl", "x"), split_axis=0, concat_axis=0, tiled=True)
    q_pieces = regroup(small(q_send_kernel, (piece,) * 4, 1)(sc, queries))
    q0 = small(join_kernel, jax.ShapeDtypeStruct((4, STRIP, 8 * DH), bf16), 4, False)(*q_pieces)
    q1 = lax.ppermute(q0, "c", swap)
    chunk = prep(kv)

    fwd, bwd = [chunk], [chunk]
    for _ in range(1, 4):
        fwd.append(lax.ppermute(fwd[-1], "z", up))
        bwd.append(lax.ppermute(bwd[-1], "z", down))
    far_l = lax.ppermute(fwd[3][:HALF], "z", up)
    far_h = lax.ppermute(bwd[3][HALF:], "z", down)

    state = own_step(sc, q0, q1, chunk)
    for k in range(1, 4):
        parts = (((0, 1), 2 + k), ((0, 1), 6 + k))
        state = ring_step(sc, (q0, q1), state, (fwd[k], bwd[k]), parts)
    far = ((far_l, far_h), (((0,), 6), ((1,), 6)))
    (theirs,) = ring_step(sc, (q1,), state[1:], *far)
    other = lax.ppermute(theirs, "c", swap)
    (ours,) = ring_step(sc, (q0,), state[:1], *far)
    pieces = small(merge_kernel, (piece,) * 4, 2)(sc, ours, other)
    out = jax.ShapeDtypeStruct((STRIP, H * DH), bf16)
    sems = [pltpu.SemaphoreType.DMA((4,))]
    return small(place_kernel, out, 4, True, VMEM, ANY, sems)(sc, *regroup(pieces))


def solution(mesh):
    fine = Mesh(mesh.devices.reshape(2, 8, 2, 4, 2), AXES)
    return jax.shard_map(
        per_device,
        mesh=fine,
        in_specs=(P(AXES, None),) * 3,
        out_specs=P(AXES, None),
        check_vma=False,
    )
```
